512 devices in a mesh: rep: 32 (over z, core), mdl: 16 (over y, x).
Axes of the slice: x: 4, y: 4, z: 16, core: 2. Of those that a mesh axis runs over, the one named last changes fastest.
Arguments:
- deltas: bfloat16 [32, 2560, 2560], P('rep', 'mdl'), may hold values from -72 to 72
- errors: bfloat16 [32, 2560, 2560], P('rep', 'mdl'), may hold values from -3 to 3
- starts: float32 [2560, 64], replicated, may hold values from -6 to 6
- momentum: float32 [2560, 2560], P('mdl', 'rep'), may hold values from -2 to 2
Outputs:
- new_errors: bfloat16 [32, 2560, 2560], P('rep', 'mdl')
- new_momentum: float32 [2560, 2560], P('mdl', 'rep')
- outer_step: float32 [2560, 2560], P('mdl', 'rep')
The draws below stay inside these ranges and needn't reach their ends.
All inputs are finite; a program needn't handle non-finite values.
Results may differ from the reference program's by a relative error of at most 0.001.
Values sent between devices are 32-bit elements; how exact they have to be, the bound alone decides.
No kernel may reach another device: no remote copies, remote signals or barrier semaphores. Data moves between devices by JAX's collectives and lax.ppermute only.
A program may use at most 64 MiB of HBM per device.

```python
import math
import jax
import jax.numpy as jnp
from jax import lax

CHANNELS = 2560
RANK = 64
REPLICAS = 32


def draw_deltas(key, part):
    keys = jax.random.split(jax.random.fold_in(key, 7), 5)
    shape_one = (CHANNELS, CHANNELS)
    common = jax.random.truncated_normal(keys[0], -4.0, 4.0, shape_one, jnp.float32)
    own = jax.random.truncated_normal(keys[1], -4.0, 4.0, (REPLICAS,) + shape_one, jnp.float32)
    ramp = 1.0 + 2.0 * jnp.arange(REPLICAS, dtype=jnp.float32) / max(REPLICAS - 1, 1)
    replica_scale = ramp * jax.random.uniform(keys[2], (REPLICAS,), jnp.float32, 0.8, 1.2)
    row_ramp = jnp.exp(math.log(3.0) * jnp.arange(CHANNELS, dtype=jnp.float32) / CHANNELS)
    row_scale = jnp.exp(jax.random.uniform(keys[3], (CHANNELS, 1), jnp.float32, math.log(0.3), 0.0)) * row_ramp[:, None]
    column_scale = jnp.exp(jax.random.uniform(keys[4], (1, CHANNELS), jnp.float32, math.log(0.3), math.log(3.0)))
    mixed = 0.3 * common[None] + replica_scale[:, None, None] * own
    return (0.5 * mixed * row_scale[None] * column_scale[None]).astype(jnp.bfloat16)


def block_scale(key, extent, shards, least, high):
    gain, own = 1.0, jax.random.fold_in(key, 6)
    for dim, parts in shards:
        heights = jnp.exp(jax.random.uniform(jax.random.fold_in(own, dim), (parts,), jnp.float32, least / len(shards), high / len(shards)))
        gain = gain * jnp.repeat(heights, extent[dim] // parts).reshape([-1 if axis == dim else 1 for axis in range(len(extent))])
    return gain


def scatter_about(own_key, extent, spread, most, cuts=(), kind=jnp.bfloat16):
    values = jax.random.normal(own_key, extent, jnp.float32) * spread
    if len(cuts) > 0:
        values = block_scale(own_key, extent, cuts, -0.22, 0.18) * values
    return jnp.clip(values, min=-most, max=most).astype(kind)


def setup_inputs(seed: int = 0) -> dict:
    arg_keys = jax.random.split(jax.random.key(seed), 5)
    deltas = draw_deltas(jax.random.fold_in(arg_keys[4], 71), 0)
    errors = scatter_about(arg_keys[1], (REPLICAS, CHANNELS, CHANNELS), 0.5, 3.0, ((0, 32), (1, 16)))
    starts = scatter_about(arg_keys[2], (CHANNELS, RANK), 1.0, 6.0, (), jnp.float32)
    momentum = scatter_about(arg_keys[3], (CHANNELS, CHANNELS), 0.3, 2.0, ((0, 16), (1, 32)), jnp.float32)
    return {"deltas": deltas, "errors": errors, "starts": starts, "momentum": momentum}


def reference(deltas, errors, starts, momentum):
    highest = lax.Precision.HIGHEST

    def left_add(total, pair):
        merged = pair[0].astype(jnp.float32) + pair[1].astype(jnp.float32)
        return (total + jnp.einsum('ac,ck->ka', merged, starts, precision=highest), None)
    left, unused = lax.scan(left_add, jnp.zeros((RANK, CHANNELS), jnp.float32), (deltas, errors))
    left = left / REPLICAS
    gram = jnp.einsum('ka,la->kl', left, left, precision=highest)
    lower = jnp.linalg.cholesky(gram)
    basis = jax.scipy.linalg.solve_triangular(lower, left, lower=True)

    def right_add(total, pair):
        merged = pair[0].astype(jnp.float32) + pair[1].astype(jnp.float32)
        return (total + jnp.einsum('ac,ka->kc', merged, basis, precision=highest), None)
    right, unused = lax.scan(right_add, jnp.zeros((RANK, CHANNELS), jnp.float32), (deltas, errors))
    right = right / REPLICAS
    approx = jnp.einsum('ka,kc->ac', basis, right, precision=highest)

    def residue(pair):
        merged = pair[0].astype(jnp.float32) + pair[1].astype(jnp.float32)
        return (merged - approx).astype(jnp.bfloat16)
    new_errors = lax.map(residue, (deltas, errors))
    new_momentum = 0.9 * momentum + approx
    outer_step = 0.7 * (approx + 0.9 * new_momentum)
    return (new_errors, new_momentum, outer_step)
```

```python
import jax
import jax.numpy as jnp
from jax import lax
from jax.sharding import Mesh
from jax.sharding import PartitionSpec as P

REP = ("far", "near", "core")
PAIR = ("near", "core")
WIDE = ("near", "core", "mdl")


highest = lax.Precision.HIGHEST


def to_each(shard, axes):
    count = lax.axis_size(axes)
    return lax.all_to_all(
        jnp.broadcast_to(shard[None], (count, *shard.shape)), axes, 0, 0, tiled=True
    )


def spread_sum(shard, near, far):
    count = lax.axis_size(near)
    tiles = shard.reshape(count, shard.shape[0] // count, shard.shape[1])
    own = lax.all_to_all(tiles, near, 0, 0, tiled=True).sum(axis=0)
    own = to_each(own, far).sum(axis=0)
    return to_each(own, near).reshape(shard.shape)


def body(deltas, errors, starts, momentum):
    replicas = lax.axis_size(REP)
    merged = deltas[0].astype(jnp.float32) + errors[0].astype(jnp.float32)
    left_part = jnp.einsum("ac,ck->ka", merged, starts, precision=highest)
    left = spread_sum(left_part, PAIR, "far") / replicas
    right_part = jnp.einsum("ac,ka->kc", merged, left, precision=highest)
    right = spread_sum(right_part, WIDE, "far") / replicas
    gram = jnp.einsum("ck,lc->kl", starts, right, precision=highest)
    lower = jnp.linalg.cholesky(gram)
    inverse = jax.scipy.linalg.solve_triangular(
        lower, jnp.eye(lower.shape[0], dtype=jnp.float32), lower=True
    )
    basis = jnp.einsum("kl,la->ka", inverse, left, precision=highest)
    turned = jnp.einsum("kl,ka->la", inverse, basis, precision=highest)
    approx = jnp.einsum("ka,kc->ac", turned, right, precision=highest)
    new_errors = (merged - approx).astype(jnp.bfloat16)[None]
    width = momentum.shape[1]
    owned = lax.dynamic_slice_in_dim(approx, lax.axis_index(REP) * width, width, 1)
    new_momentum = 0.9 * momentum + owned
    outer_step = 0.7 * (owned + 0.9 * new_momentum)
    return (new_errors, new_momentum, outer_step)


def solution(mesh):
    torus = Mesh(mesh.devices.reshape(8, 2, 2, 16), ("far", "near", "core", "mdl"))
    in_specs = (P(REP, "mdl", None), P(REP, "mdl", None), P(), P("mdl", REP))
    out_specs = (P(REP, "mdl", None), P("mdl", REP), P("mdl", REP))
    return jax.shard_map(body, mesh=torus, in_specs=in_specs, out_specs=out_specs, check_vma=False)
```

```python
import jax
import jax.numpy as jnp
from jax import lax
from jax.sharding import Mesh
from jax.sharding import PartitionSpec as P

REP = ("far", "near", "core")
PAIR = ("near", "core")
WIDE = ("near", "core", "mdl")


highest = lax.Precision.HIGHEST


def to_each(shard, axes):
    count = lax.axis_size(axes)
    return lax.all_to_all(
        jnp.broadcast_to(shard[None], (count, *shard.shape)), axes, 0, 0, tiled=True
    )


def left_sum(part):
    rank, rows = part.shape
    count = lax.axis_size(PAIR)
    own = lax.all_to_all(part.reshape(count, rank // count, rows), PAIR, 0, 0, tiled=True)
    own = to_each(own.sum(axis=0), "far").sum(axis=0) / lax.axis_size(REP)
    return to_each(own, PAIR).reshape(rank, rows)


def body(deltas, errors, starts, momentum):
    merged = deltas[0].astype(jnp.float32) + errors[0].astype(jnp.float32)
    left_part = jnp.einsum("ac,ck->ka", merged, starts, precision=highest)
    left = left_sum(left_part)
    rank = left.shape[0]
    columns = merged.shape[1]
    right_part = jnp.einsum("ac,ka->kc", merged, left, precision=highest)
    share = rank // lax.axis_size(REP)
    mine = lax.dynamic_slice_in_dim(left, lax.axis_index(REP) * share, share, 0)
    gram_part = jnp.einsum("ka,la->kl", mine, left, precision=highest).reshape(1, -1)
    load = jnp.concatenate(
        [right_part, jnp.broadcast_to(gram_part, (rank, gram_part.shape[1]))], axis=1
    )
    seen = lax.all_to_all(load, WIDE, 0, 0, tiled=True)
    row = seen[:, :columns].sum(axis=0)
    pairs = lax.axis_size(PAIR)
    lines = seen[:, columns:].reshape(pairs, -1, gram_part.shape[1]).sum(axis=1)
    far = to_each(jnp.concatenate([row, lines.reshape(-1)]), "far")
    row = far[:, :columns].sum(axis=0) / lax.axis_size(REP)
    right = to_each(row, WIDE)
    gram = far[:, columns:].reshape(rank, rank)
    lower = jnp.linalg.cholesky(gram)
    inverse = jax.scipy.linalg.solve_triangular(
        lower, jnp.eye(rank, dtype=jnp.float32), lower=True
    )
    basis = jnp.einsum("kl,la->ka", inverse, left, precision=highest)
    turned = jnp.einsum("kl,ka->la", inverse, basis, precision=highest)
    approx = jnp.einsum("ka,kc->ac", turned, right, precision=highest)
    new_errors = (merged - approx).astype(jnp.bfloat16)[None]
    width = momentum.shape[1]
    owned = lax.dynamic_slice_in_dim(approx, lax.axis_index(REP) * width, width, 1)
    new_momentum = 0.9 * momentum + owned
    outer_step = 0.7 * (owned + 0.9 * new_momentum)
    return (new_errors, new_momentum, outer_step)


def solution(mesh):
    torus = Mesh(mesh.devices.reshape(8, 2, 2, 16), ("far", "near", "core", "mdl"))
    in_specs = (P(REP, "mdl", None), P(REP, "mdl", None), P(), P("mdl", REP))
    out_specs = (P(REP, "mdl", None), P("mdl", REP), P("mdl", REP))
    return jax.shard_map(body, mesh=torus, in_specs=in_specs, out_specs=out_specs, check_vma=False)
```

```python
import jax
import jax.numpy as jnp
from jax import lax
from jax.experimental import pallas as pl
from jax.experimental.pallas import tpu as pltpu
from jax.sharding import Mesh
from jax.sharding import PartitionSpec as P

REP = ("far", "near", "core")
PAIR = ("near", "core")
WIDE = ("near", "core", "mdl")
CHUNKS = 4


highest = lax.Precision.HIGHEST
ANY = pl.BlockSpec(memory_space=pl.ANY)
VMEM = pl.BlockSpec(memory_space=pltpu.VMEM)
SMEM = pl.BlockSpec(memory_space=pltpu.SMEM)


def held(shape):
    return pltpu.VMEM(shape, jnp.float32)


def near_core(values):
    return pltpu.with_memory_space_constraint(values, pltpu.VMEM)


def pieces_of(values, count):
    found = []
    for _ in range(count):
        piece = values.astype(jnp.bfloat16)
        found.append(piece)
        values = values - piece.astype(jnp.float32)
    return found


def dot(a, b, dims):
    return lax.dot_general(a, b, (dims, ((), ())), preferred_element_type=jnp.float32)


def folded(stack, count):
    rows = stack.shape[0] // count
    return sum(stack[i * rows : (i + 1) * rows] for i in reversed(range(count)))


def left_kernel(deltas, errors, starts, out, d_buf, e_buf, s_buf, sems):
    width = d_buf.shape[1] // CHUNKS
    copies = []
    for j in range(CHUNKS):
        cut = pl.ds(j * width, width)
        three = (
            pltpu.make_async_copy(starts.at[:, cut], s_buf.at[:, cut], sems.at[j, 0]),
            pltpu.make_async_copy(deltas.at[0, :, cut], d_buf.at[:, cut], sems.at[j, 1]),
            pltpu.make_async_copy(errors.at[0, :, cut], e_buf.at[:, cut], sems.at[j, 2]),
        )
        for copy in three:
            copy.start()
        copies.append(three)
    total = None
    for j in range(CHUNKS):
        cut = slice(j * width, (j + 1) * width)
        copies[j][0].wait()
        stack = jnp.concatenate(pieces_of(s_buf[:, cut], 3), axis=0)
        copies[j][1].wait()
        part = dot(stack, d_buf[:, cut], ((1,), (1,)))
        copies[j][2].wait()
        part = part + dot(stack, e_buf[:, cut], ((1,), (1,)))
        total = part if total is None else total + part
    out[...] = folded(total, 3).reshape(out.shape)


def left_part_of(deltas, errors, starts):
    rows, columns = deltas.shape[1:]
    rank = starts.shape[0]
    count = lax.axis_size(PAIR)
    return pl.pallas_call(
        left_kernel,
        out_shape=held((count, rank // count, rows)),
        in_specs=[ANY, ANY, ANY],
        out_specs=VMEM,
        scratch_shapes=[
            pltpu.VMEM((rows, columns), jnp.bfloat16),
            pltpu.VMEM((rows, columns), jnp.bfloat16),
            pltpu.VMEM((rank, columns), jnp.float32),
            pltpu.SemaphoreType.DMA((CHUNKS, 3)),
        ],
        name="left_part",
    )(deltas, errors, starts)


def gram_line(left, place):
    rank = left.shape[0]
    share = 128 // rank
    index = lax.broadcasted_iota(jnp.int32, left.shape, 0)
    nothing = jnp.zeros_like(left)
    line = None
    for i in range(share):
        own = jnp.sum(jnp.where(index == place * share + i, left, nothing), axis=0, keepdims=True)
        lanes = jnp.concatenate([nothing] * i + [left] + [nothing] * (share - 1 - i), axis=0)
        part = lax.dot_general(
            own, lanes, (((1,), (1,)), ((), ())), precision=highest, preferred_element_type=jnp.float32
        )
        line = part if line is None else line + part
    return line


def right_kernel(place, left, deltas, errors, out):
    columns = deltas.shape[2]
    width = columns // CHUNKS
    rank = left.shape[0] * left.shape[1]
    whole = left[...].reshape(rank, left.shape[2])
    line = gram_line(whole, place[0])
    stack = jnp.concatenate(pieces_of(whole, 3), axis=0)
    for j in range(CHUNKS):
        cut = slice(j * width, (j + 1) * width)
        part = dot(stack, deltas[0, :, cut], ((1,), (0,)))
        part = part + dot(stack, errors[0, :, cut], ((1,), (0,)))
        out[:, 0, cut] = folded(part, 3)
    out[:, 0, columns:] = jnp.broadcast_to(line, (rank, line.shape[1]))


def right_part_of(place, left, deltas, errors):
    rank = left.shape[0] * left.shape[1]
    columns = deltas.shape[2]
    return pl.pallas_call(
        right_kernel,
        out_shape=held((rank, 1, columns + 128)),
        in_specs=[SMEM, VMEM, VMEM, VMEM],
        out_specs=VMEM,
        name="right_part",
    )(place, near_core(left), near_core(deltas), near_core(errors))


def out_kernel(place, turned, flipped, right, deltas, errors, momentum, new_errors, new_momentum, outer_step, buf, sems):
    columns = right.shape[2]
    owned = momentum.shape[1]
    width = columns // CHUNKS
    copies = []
    for j in range(CHUNKS):
        cut = slice(j * width, (j + 1) * width)
        big, small = pieces_of(right[:, 0, cut], 2)
        approx = dot(flipped[...], jnp.concatenate([big, small, big, small], axis=0), ((1,), (0,)))
        merged = deltas[0, :, cut].astype(jnp.float32) + errors[0, :, cut].astype(jnp.float32)
        buf[:, cut] = (merged - approx).astype(jnp.bfloat16)
        cut = pl.ds(j * width, width)
        copy = pltpu.make_async_copy(buf.at[:, cut], new_errors.at[0, :, cut], sems.at[j])
        copy.start()
        copies.append(copy)
    first = place[0] * owned
    base = jnp.minimum(first // 128, columns // 128 - 2) * 128
    window = right[:, 0, pl.ds(pl.multiple_of(base, 128), 256)]
    window = pltpu.roll(window, lax.rem(256 - (first - base), 256), 1)[:, :128]
    mine = lax.dot_general(
        turned[...], window, (((0,), (0,)), ((), ())), precision=highest, preferred_element_type=jnp.float32
    )[:, :owned]
    fresh = 0.9 * momentum[...] + mine
    new_momentum[...] = fresh
    outer_step[...] = 0.7 * (mine + 0.9 * fresh)
    for copy in copies:
        copy.wait()


def outputs_of(place, turned, right, deltas, errors, momentum):
    big, small = pieces_of(turned, 2)
    flipped = jnp.concatenate([big, big, small, small], axis=0).T
    f32 = jnp.float32
    return pl.pallas_call(
        out_kernel,
        out_shape=(
            jax.ShapeDtypeStruct(deltas.shape, jnp.bfloat16),
            jax.ShapeDtypeStruct(momentum.shape, f32),
            jax.ShapeDtypeStruct(momentum.shape, f32),
        ),
        in_specs=[SMEM, VMEM, VMEM, VMEM, VMEM, VMEM, VMEM],
        out_specs=(ANY, VMEM, VMEM),
        scratch_shapes=[
            pltpu.VMEM(deltas.shape[1:], jnp.bfloat16),
            pltpu.SemaphoreType.DMA((CHUNKS,)),
        ],
        name="outputs",
    )(place, near_core(turned), near_core(flipped), near_core(right), near_core(deltas), near_core(errors), near_core(momentum))


def to_each(shard, axes):
    count = lax.axis_size(axes)
    return lax.all_to_all(
        jnp.broadcast_to(shard[None], (count, *shard.shape)), axes, 0, 0, tiled=True
    )


def body(deltas, errors, starts, momentum):
    replicas = lax.axis_size(REP)
    rank = starts.shape[1]
    columns = deltas.shape[2]
    place = lax.axis_index(REP)[None]
    left_part, place = lax.optimization_barrier((left_part_of(deltas, errors, starts.T), place))
    own = lax.all_to_all(left_part, PAIR, 0, 0, tiled=True).sum(axis=0)
    own = to_each(own, "far").sum(axis=0) / replicas
    tiles = to_each(own, PAIR)
    left = tiles.reshape(rank, -1)
    load = right_part_of(place, tiles, deltas, errors)
    seen = lax.all_to_all(load, WIDE, 0, 0, tiled=True)
    row = seen[:, :, :columns].sum(axis=0)
    pairs = lax.axis_size(PAIR)
    lines = seen[:, 0, columns:].reshape(pairs, -1, 128).sum(axis=1)
    far = to_each(jnp.concatenate([row, lines.reshape(1, -1)], axis=1), "far")
    row = far[:, :, :columns].sum(axis=0) / replicas
    right = to_each(row, WIDE)
    gram = far[:, 0, columns:].reshape(rank, rank)
    lower = jnp.linalg.cholesky(gram)
    inverse = jax.scipy.linalg.solve_triangular(
        lower, jnp.eye(rank, dtype=jnp.float32), lower=True
    )
    basis = jnp.einsum("kl,la->ka", inverse, left, precision=highest)
    turned = jnp.einsum("kl,ka->la", inverse, basis, precision=highest)
    return outputs_of(place, turned, right, deltas, errors, momentum)


def solution(mesh):
    torus = Mesh(mesh.devices.reshape(8, 2, 2, 16), ("far", "near", "core", "mdl"))
    in_specs = (P(REP, "mdl", None), P(REP, "mdl", None), P(), P("mdl", REP))
    out_specs = (P(REP, "mdl", None), P("mdl", REP), P("mdl", REP))
    return jax.shard_map(body, mesh=torus, in_specs=in_specs, out_specs=out_specs, check_vma=False)
```

```python
import jax
import jax.numpy as jnp
from jax import lax
from jax.experimental import pallas as pl
from jax.experimental.pallas import tpu as pltpu
from jax.sharding import Mesh
from jax.sharding import PartitionSpec as P

REP = ("far", "near", "core")
PAIR = ("near", "core")
NODES = ("near", "mdl")
WIDE = ("core", "near", "mdl")
CHUNKS = 4


highest = lax.Precision.HIGHEST
ANY = pl.BlockSpec(memory_space=pl.ANY)
HBM = pl.BlockSpec(memory_space=pltpu.HBM)
VMEM = pl.BlockSpec(memory_space=pltpu.VMEM)
SMEM = pl.BlockSpec(memory_space=pltpu.SMEM)
SMALL = pltpu.CompilerParams(vmem_limit_bytes=24 << 20)


def held(shape):
    return pltpu.VMEM(shape, jnp.float32)


def near_core(values):
    return pltpu.with_memory_space_constraint(values, pltpu.VMEM)


def far_off(values):
    return pltpu.with_memory_space_constraint(values, pltpu.HBM)


def pieces_of(values, count):
    found = []
    for _ in range(count):
        piece = values.astype(jnp.bfloat16)
        found.append(piece)
        values = values - piece.astype(jnp.float32)
    return found


def dot(a, b, dims):
    return lax.dot_general(a, b, (dims, ((), ())), preferred_element_type=jnp.float32)


def folded(stack, count):
    rows = stack.shape[0] // count
    return sum(stack[i * rows : (i + 1) * rows] for i in reversed(range(count)))


def left_kernel(place, deltas, errors, starts, out, partner, d_buf, e_buf, s_buf, sems):
    width = d_buf.shape[1] // CHUNKS
    copies = []
    for j in range(CHUNKS):
        cut = pl.ds(j * width, width)
        three = (
            pltpu.make_async_copy(starts.at[:, cut], s_buf.at[:, cut], sems.at[j, 0]),
            pltpu.make_async_copy(deltas.at[0, :, cut], d_buf.at[:, cut], sems.at[j, 1]),
            pltpu.make_async_copy(errors.at[0, :, cut], e_buf.at[:, cut], sems.at[j, 2]),
        )
        for copy in three:
            copy.start()
        copies.append(three)
    total = None
    for j in range(CHUNKS):
        cut = slice(j * width, (j + 1) * width)
        copies[j][0].wait()
        stack = jnp.concatenate(pieces_of(s_buf[:, cut], 3), axis=0)
        copies[j][1].wait()
        part = dot(stack, d_buf[:, cut], ((1,), (1,)))
        copies[j][2].wait()
        part = part + dot(stack, e_buf[:, cut], ((1,), (1,)))
        total = part if total is None else total + part
    share = partner.shape[1]
    cut = pl.ds(pl.multiple_of((1 - place[0] % 2) * share, 128), share)
    partner[...] = d_buf[:, cut].astype(jnp.float32) + e_buf[:, cut].astype(jnp.float32)
    out[...] = folded(total, 3).reshape(out.shape)


def left_part_of(place, deltas, errors, starts):
    rows, columns = deltas.shape[1:]
    rank = starts.shape[0]
    count = lax.axis_size(PAIR)
    return pl.pallas_call(
        left_kernel,
        out_shape=(
            held((count, rank // count, rows)),
            held((rows, columns // 2)),
        ),
        in_specs=[SMEM, HBM, HBM, HBM],
        out_specs=(VMEM, VMEM),
        scratch_shapes=[
            pltpu.VMEM((rows, columns), jnp.bfloat16),
            pltpu.VMEM((rows, columns), jnp.bfloat16),
            held((rank, columns)),
            pltpu.SemaphoreType.DMA((CHUNKS, 3)),
        ],
        compiler_params=SMALL,
        name="left_part",
    )(place, far_off(deltas), far_off(errors), far_off(starts))


def gram_lines(left, first, count):
    rank = left.shape[0]
    share = 128 // rank
    index = lax.broadcasted_iota(jnp.int32, left.shape, 0)
    nothing = jnp.zeros_like(left)
    lines = None
    for i in range(share):
        own = jnp.concatenate(
            [
                jnp.sum(jnp.where(index == first + share * n + i, left, nothing), axis=0, keepdims=True)
                for n in range(count)
            ],
            axis=0,
        )
        lanes = jnp.concatenate([nothing] * i + [left] + [nothing] * (share - 1 - i), axis=0)
        part = lax.dot_general(
            own, lanes, (((1,), (1,)), ((), ())), precision=highest, preferred_element_type=jnp.float32
        )
        lines = part if lines is None else lines + part
    return lines


def right_kernel(place, left, partner, deltas, errors, out):
    columns = partner.shape[1]
    chunks = CHUNKS // 2
    width = columns // chunks
    rank = left.shape[0] * left.shape[1]
    whole = left[...].reshape(rank, left.shape[2])
    stack = jnp.concatenate(pieces_of(whole, 3), axis=0)
    base = place[0] % 2 * columns
    for j in range(chunks):
        cut = slice(j * width, (j + 1) * width)
        own = pl.ds(pl.multiple_of(base + j * width, 128), width)
        merged = deltas[0, :, own].astype(jnp.float32) + errors[0, :, own].astype(jnp.float32)
        pieces = pieces_of(merged + partner[:, cut], 3)
        part = None
        for piece in reversed(pieces):
            term = dot(stack, piece, ((1,), (0,)))
            part = term if part is None else part + term
        out[:, 0, cut] = folded(part, 3)
    lines = gram_lines(whole, place[0] // 2 * 4, 2)
    parity = lax.broadcasted_iota(jnp.int32, (rank, lines.shape[1]), 0) % 2
    out[:, 0, columns:] = jnp.where(parity == 0, lines[0:1], lines[1:2])


def right_part_of(place, left, partner, deltas, errors):
    rank = left.shape[0] * left.shape[1]
    return pl.pallas_call(
        right_kernel,
        out_shape=held((rank, 1, partner.shape[1] + 128)),
        in_specs=[SMEM, VMEM, VMEM, VMEM, VMEM],
        out_specs=VMEM,
        compiler_params=SMALL,
        name="right_part",
    )(place, near_core(left), near_core(partner), near_core(deltas), near_core(errors))


def out_kernel(place, turned, flipped, right, deltas, errors, momentum, new_errors, new_momentum, outer_step, buf, fresh, step, sems):
    half = right.shape[3]
    owned = momentum.shape[1]
    each = half // owned
    first = place[0] % each * owned
    base = pl.multiple_of(jnp.minimum(first // 128, half // 128 - 2) * 128, 128)
    window = right[place[0] // each, :, 0, pl.ds(base, 256)]
    window = pltpu.roll(window, lax.rem(256 - (first - base), 256), 1)[:, :128]
    mine = lax.dot_general(
        turned[...], window, (((0,), (0,)), ((), ())), precision=highest, preferred_element_type=jnp.float32
    )[:, :owned]
    fresh[...] = 0.9 * momentum[...] + mine
    step[...] = 0.7 * (mine + 0.9 * fresh[...])
    copies = [
        pltpu.make_async_copy(fresh, new_momentum, sems.at[CHUNKS]),
        pltpu.make_async_copy(step, outer_step, sems.at[CHUNKS + 1]),
    ]
    for copy in copies:
        copy.start()
    width = 2 * half // CHUNKS
    for j in range(CHUNKS):
        side, start = divmod(j * width, half)
        big, small = pieces_of(right[side, :, 0, start : start + width], 2)
        approx = dot(flipped[...], jnp.concatenate([big, small, big, small], axis=0), ((1,), (0,)))
        cut = pl.ds(j * width, width)
        merged = deltas[0, :, cut].astype(jnp.float32) + errors[0, :, cut].astype(jnp.float32)
        buf[:, cut] = (merged - approx).astype(jnp.bfloat16)
        copy = pltpu.make_async_copy(buf.at[:, cut], new_errors.at[0, :, cut], sems.at[j])
        copy.start()
        copies.append(copy)
    for copy in copies:
        copy.wait()


def outputs_of(place, turned, right, deltas, errors, momentum):
    big, small = pieces_of(turned, 2)
    flipped = jnp.concatenate([big, big, small, small], axis=0).T
    f32 = jnp.float32
    return pl.pallas_call(
        out_kernel,
        out_shape=(
            jax.ShapeDtypeStruct(deltas.shape, jnp.bfloat16),
            jax.ShapeDtypeStruct(momentum.shape, f32),
            jax.ShapeDtypeStruct(momentum.shape, f32),
        ),
        in_specs=[SMEM, VMEM, VMEM, VMEM, VMEM, VMEM, VMEM],
        out_specs=(HBM, HBM, HBM),
        scratch_shapes=[
            pltpu.VMEM(deltas.shape[1:], jnp.bfloat16),
            held(momentum.shape),
            held(momentum.shape),
            pltpu.SemaphoreType.DMA((CHUNKS + 2,)),
        ],
        compiler_params=SMALL,
        name="outputs",
    )(place, near_core(turned), near_core(flipped), near_core(right), near_core(deltas), near_core(errors), near_core(momentum))


def to_each(shard, axes):
    count = lax.axis_size(axes)
    return lax.all_to_all(
        jnp.broadcast_to(shard[None], (count, *shard.shape)), axes, 0, 0, tiled=True
    )


def body(deltas, errors, starts, momentum):
    replicas = lax.axis_size(REP)
    rank = starts.shape[1]
    columns = deltas.shape[2]
    place = lax.axis_index(REP)[None]
    left_part, other = left_part_of(place, deltas, errors, starts.T)
    own = lax.all_to_all(left_part, PAIR, 0, 0, tiled=True).sum(axis=0)
    partner = lax.ppermute(other, "core", [(0, 1), (1, 0)])
    own = to_each(own, "far").sum(axis=0) / replicas
    own, partner = lax.optimization_barrier((own, partner))
    tiles = to_each(own, PAIR)
    left = tiles.reshape(rank, -1)
    load = right_part_of(place, tiles, partner, deltas, errors)
    half = columns // 2
    nodes = lax.axis_size(NODES)
    load = load.reshape(nodes, rank // nodes, 1, -1)
    seen = lax.all_to_all(load, NODES, 0, 0, tiled=True)
    row = seen[..., :half].sum(axis=0)
    lines = seen[..., half:].reshape(lax.axis_size("near"), -1, rank // nodes, 128).sum(axis=1)
    far = to_each(jnp.concatenate([row.reshape(1, -1), lines.reshape(1, -1)], axis=1), "far")
    row = far[:, :, :columns].sum(axis=0) / replicas
    right = to_each(row, WIDE).reshape(2, rank, 1, half)
    gram = far[:, 0, columns:].reshape(rank, rank)
    lower = jnp.linalg.cholesky(gram)
    inverse = jax.scipy.linalg.solve_triangular(
        lower, jnp.eye(rank, dtype=jnp.float32), lower=True
    )
    basis = jnp.einsum("kl,la->ka", inverse, left, precision=highest)
    turned = jnp.einsum("kl,ka->la", inverse, basis, precision=highest)
    return outputs_of(place, turned, right, deltas, errors, momentum)


def solution(mesh):
    torus = Mesh(mesh.devices.reshape(8, 2, 2, 16), ("far", "near", "core", "mdl"))
    in_specs = (P(REP, "mdl", None), P(REP, "mdl", None), P(), P("mdl", REP))
    out_specs = (P(REP, "mdl", None), P("mdl", REP), P("mdl", REP))
    return jax.shard_map(body, mesh=torus, in_specs=in_specs, out_specs=out_specs, check_vma=False)
```

```python
import jax
import jax.numpy as jnp
from jax import lax
from jax.experimental import pallas as pl
from jax.experimental.pallas import tpu as pltpu
from jax.sharding import Mesh
from jax.sharding import PartitionSpec as P

REP = ("far", "near", "core")
PAIR = ("near", "core")
NODES = ("near", "mdl")
SWAP = [(0, 1), (1, 0)]
CHUNKS = 4
BLOCK = 4


highest = lax.Precision.HIGHEST
ANY = pl.BlockSpec(memory_space=pl.ANY)
HBM = pl.BlockSpec(memory_space=pltpu.HBM)
VMEM = pl.BlockSpec(memory_space=pltpu.VMEM)
SMEM = pl.BlockSpec(memory_space=pltpu.SMEM)
SMALL = pltpu.CompilerParams(vmem_limit_bytes=24 << 20)


def held(shape):
    return pltpu.VMEM(shape, jnp.float32)


def near_core(values):
    return pltpu.with_memory_space_constraint(values, pltpu.VMEM)


def far_off(values):
    return pltpu.with_memory_space_constraint(values, pltpu.HBM)


def pieces_of(values, count):
    found = []
    for _ in range(count):
        piece = values.astype(jnp.bfloat16)
        found.append(piece)
        values = values - piece.astype(jnp.float32)
    return found


def dot(a, b, dims):
    return lax.dot_general(a, b, (dims, ((), ())), preferred_element_type=jnp.float32)


def folded(stack, count):
    rows = stack.shape[0] // count
    return sum(stack[i * rows : (i + 1) * rows] for i in reversed(range(count)))


def left_kernel(place, deltas, errors, starts, out, partner, d_buf, e_buf, s_buf, sems):
    width = d_buf.shape[1] // CHUNKS
    copies = []
    for j in range(CHUNKS):
        cut = pl.ds(j * width, width)
        three = (
            pltpu.make_async_copy(starts.at[:, cut], s_buf.at[:, cut], sems.at[j, 0]),
            pltpu.make_async_copy(deltas.at[0, :, cut], d_buf.at[:, cut], sems.at[j, 1]),
            pltpu.make_async_copy(errors.at[0, :, cut], e_buf.at[:, cut], sems.at[j, 2]),
        )
        for copy in three:
            copy.start()
        copies.append(three)
    total = None
    for j in range(CHUNKS):
        cut = slice(j * width, (j + 1) * width)
        copies[j][0].wait()
        stack = jnp.concatenate(pieces_of(s_buf[:, cut], 3), axis=0)
        copies[j][1].wait()
        part = dot(stack, d_buf[:, cut], ((1,), (1,)))
        copies[j][2].wait()
        part = part + dot(stack, e_buf[:, cut], ((1,), (1,)))
        total = part if total is None else total + part
    share = partner.shape[1]
    cut = pl.ds(pl.multiple_of((1 - place[0] % 2) * share, 128), share)
    partner[...] = d_buf[:, cut].astype(jnp.float32) + e_buf[:, cut].astype(jnp.float32)
    out[...] = folded(total, 3).reshape(out.shape)


def left_part_of(place, deltas, errors, starts):
    rows, columns = deltas.shape[1:]
    rank = starts.shape[0]
    count = lax.axis_size(PAIR)
    return pl.pallas_call(
        left_kernel,
        out_shape=(
            held((count, rank // count, rows)),
            held((rows, columns // 2)),
        ),
        in_specs=[SMEM, HBM, HBM, HBM],
        out_specs=(VMEM, VMEM),
        scratch_shapes=[
            pltpu.VMEM((rows, columns), jnp.bfloat16),
            pltpu.VMEM((rows, columns), jnp.bfloat16),
            held((rank, columns)),
            pltpu.SemaphoreType.DMA((CHUNKS, 3)),
        ],
        compiler_params=SMALL,
        name="left_part",
    )(place, far_off(deltas), far_off(errors), far_off(starts))


def gram_lines(left, first, count):
    rank = left.shape[0]
    share = 128 // rank
    index = lax.broadcasted_iota(jnp.int32, left.shape, 0)
    nothing = jnp.zeros_like(left)
    lines = None
    for i in range(share):
        own = jnp.concatenate(
            [
                jnp.sum(jnp.where(index == first + share * n + i, left, nothing), axis=0, keepdims=True)
                for n in range(count)
            ],
            axis=0,
        )
        lanes = jnp.concatenate([nothing] * i + [left] + [nothing] * (share - 1 - i), axis=0)
        part = lax.dot_general(
            own, lanes, (((1,), (1,)), ((), ())), precision=highest, preferred_element_type=jnp.float32
        )
        lines = part if lines is None else lines + part
    return lines


def right_kernel(place, left, partner, deltas, errors, out):
    columns = partner.shape[1]
    chunks = CHUNKS // 2
    width = columns // chunks
    rank = left.shape[0] * left.shape[1]
    whole = left[...].reshape(rank, left.shape[2])
    stack = jnp.concatenate(pieces_of(whole, 3), axis=0)
    base = place[0] % 2 * columns
    for j in range(chunks):
        cut = slice(j * width, (j + 1) * width)
        own = pl.ds(pl.multiple_of(base + j * width, 128), width)
        merged = deltas[0, :, own].astype(jnp.float32) + errors[0, :, own].astype(jnp.float32)
        pieces = pieces_of(merged + partner[:, cut], 3)
        part = None
        for piece in reversed(pieces):
            term = dot(stack, piece, ((1,), (0,)))
            part = term if part is None else part + term
        out[:, 0, cut] = folded(part, 3)
    lines = gram_lines(whole, place[0] // 2 * 4, 2)
    parity = lax.broadcasted_iota(jnp.int32, (rank, lines.shape[1]), 0) % 2
    out[:, 0, columns:] = jnp.where(parity == 0, lines[0:1], lines[1:2])


def right_part_of(place, left, partner, deltas, errors):
    rank = left.shape[0] * left.shape[1]
    return pl.pallas_call(
        right_kernel,
        out_shape=held((rank, 1, partner.shape[1] + 128)),
        in_specs=[SMEM, VMEM, VMEM, VMEM, VMEM],
        out_specs=VMEM,
        compiler_params=SMALL,
        name="right_part",
    )(place, near_core(left), near_core(partner), near_core(deltas), near_core(errors))


def lower_inverse_of(gram):
    rank = gram.shape[0]
    ident = jnp.where(
        lax.broadcasted_iota(jnp.int32, (rank, rank), 0) == lax.broadcasted_iota(jnp.int32, (rank, rank), 1), 1.0, 0.0
    )
    table = jnp.concatenate([gram, ident], axis=1)
    index = lax.broadcasted_iota(jnp.int32, table.shape, 0)
    for k in range(0, rank, BLOCK):
        cols = [jnp.broadcast_to(table[:, k + j : k + j + 1], table.shape) for j in range(BLOCK)]
        for j in range(BLOCK):
            at = k + j
            scale = 1.0 / cols[j][at : at + 1]
            ratio = jnp.where(index > at, cols[j] * scale, 0.0)
            for n in range(j + 1, BLOCK):
                cols[n] = cols[n] - ratio * cols[n][at : at + 1]
            line = table[at : at + 1]
            table = jnp.where(index == at, line * jnp.sqrt(scale), table - ratio * line)
    lane = lax.broadcasted_iota(jnp.int32, table.shape, 1)
    return jnp.where(lane < rank, pltpu.roll(table, rank, 1), table)


def factor_kernel(gram, left, out):
    rank = gram.shape[0]
    whole = left[...].reshape(rank, left.shape[2])
    inverse = lower_inverse_of(gram[...])
    basis = lax.dot_general(
        inverse[:, :rank], whole, (((1,), (0,)), ((), ())), precision=highest, preferred_element_type=jnp.float32
    )
    twice = lax.dot_general(
        basis, inverse, (((0,), (0,)), ((), ())), precision=highest, preferred_element_type=jnp.float32
    )
    out[...] = jnp.concatenate(pieces_of(twice, 2), axis=1)


def factor_of(gram, left):
    return pl.pallas_call(
        factor_kernel,
        out_shape=pltpu.VMEM((left.shape[2], 4 * gram.shape[0]), jnp.bfloat16),
        in_specs=[VMEM, VMEM],
        out_specs=VMEM,
        compiler_params=SMALL,
        cost_estimate=pl.CostEstimate(flops=40_000_000, transcendentals=0, bytes_accessed=200_000),
        name="factor",
    )(near_core(gram), near_core(left))


def product(flipped, right):
    big, small = pieces_of(right, 2)
    return dot(flipped, jnp.concatenate([big, small, big, small], axis=0), ((1,), (0,)))


def residue(flipped, right, deltas, errors, base, j, width):
    approx = product(flipped[...], right[:, 0, j * width : (j + 1) * width])
    cut = pl.ds(pl.multiple_of(base + j * width, 128), width)
    merged = deltas[0, :, cut].astype(jnp.float32) + errors[0, :, cut].astype(jnp.float32)
    return (merged - approx).astype(jnp.bfloat16)


def near_kernel(place, flipped, right, deltas, errors, out):
    half = right.shape[2]
    width = half // (CHUNKS // 2)
    base = place[0] % 2 * half
    for j in range(CHUNKS // 2):
        out[:, j * width : (j + 1) * width] = residue(flipped, right, deltas, errors, base, j, width)


def near_half_of(place, flipped, right, deltas, errors):
    return pl.pallas_call(
        near_kernel,
        out_shape=pltpu.VMEM((deltas.shape[1], right.shape[2]), jnp.bfloat16),
        in_specs=[SMEM, VMEM, VMEM, VMEM, VMEM],
        out_specs=VMEM,
        compiler_params=SMALL,
        cost_estimate=pl.CostEstimate(flops=40_000_000, transcendentals=0, bytes_accessed=2_000_000),
        name="near_half",
    )(place, near_core(flipped), near_core(right), near_core(deltas), near_core(errors))


def out_kernel(place, flipped, right, other, ready, deltas, errors, momentum, new_errors, new_momentum, outer_step, buf, fresh, step, sems):
    half = right.shape[2]
    owned = momentum.shape[1]
    each = half // owned
    core = place[0] % 2
    own = pl.ds(pl.multiple_of(core * half, 128), half)
    copies = [pltpu.make_async_copy(ready, new_errors.at[0, :, own], sems.at[0])]
    copies[0].start()
    first = place[0] % each * owned
    base = pl.multiple_of(jnp.minimum(first // 128, half // 128 - 2) * 128, 128)
    cut = pl.ds(base, 256)
    window = jnp.where(place[0] // each == core, right[:, 0, cut], other[:, 0, cut])
    window = pltpu.roll(window, lax.rem(256 - (first - base), 256), 1)[:, :128]
    mine = product(flipped[...], window)[:, :owned]
    fresh[...] = 0.9 * momentum[...] + mine
    step[...] = 0.7 * (mine + 0.9 * fresh[...])
    copies.append(pltpu.make_async_copy(fresh, new_momentum, sems.at[1]))
    copies.append(pltpu.make_async_copy(step, outer_step, sems.at[2]))
    for copy in copies[1:]:
        copy.start()
    width = half // (CHUNKS // 2)
    base = (1 - core) * half
    for j in range(CHUNKS // 2):
        cut = slice(j * width, (j + 1) * width)
        buf[:, cut] = residue(flipped, other, deltas, errors, base, j, width)
        there = pl.ds(pl.multiple_of(base + j * width, 128), width)
        copy = pltpu.make_async_copy(buf.at[:, pl.ds(j * width, width)], new_errors.at[0, :, there], sems.at[3 + j])
        copy.start()
        copies.append(copy)
    for copy in copies:
        copy.wait()


def outputs_of(place, flipped, right, other, ready, deltas, errors, momentum):
    f32 = jnp.float32
    return pl.pallas_call(
        out_kernel,
        out_shape=(
            jax.ShapeDtypeStruct(deltas.shape, jnp.bfloat16),
            jax.ShapeDtypeStruct(momentum.shape, f32),
            jax.ShapeDtypeStruct(momentum.shape, f32),
        ),
        in_specs=[SMEM] + [VMEM] * 7,
        out_specs=(HBM, HBM, HBM),
        scratch_shapes=[
            pltpu.VMEM(ready.shape, jnp.bfloat16),
            held(momentum.shape),
            held(momentum.shape),
            pltpu.SemaphoreType.DMA((3 + CHUNKS // 2,)),
        ],
        compiler_params=SMALL,
        name="outputs",
    )(place, *(near_core(a) for a in (flipped, right, other, ready, deltas, errors, momentum)))


def to_each(shard, axes):
    count = lax.axis_size(axes)
    return lax.all_to_all(
        jnp.broadcast_to(shard[None], (count, *shard.shape)), axes, 0, 0, tiled=True
    )


def body(deltas, errors, starts, momentum):
    replicas = lax.axis_size(REP)
    rank = starts.shape[1]
    columns = deltas.shape[2]
    place = lax.axis_index(REP)[None]
    left_part, other = left_part_of(place, deltas, errors, starts.T)
    own = lax.all_to_all(left_part, PAIR, 0, 0, tiled=True).sum(axis=0)
    partner = lax.ppermute(other, "core", SWAP)
    own = to_each(own, "far").sum(axis=0) / replicas
    own, partner = lax.optimization_barrier((own, partner))
    tiles = to_each(own, PAIR)
    load = right_part_of(place, tiles, partner, deltas, errors)
    half = columns // 2
    nodes = lax.axis_size(NODES)
    load = load.reshape(nodes, rank // nodes, 1, -1)
    seen = lax.all_to_all(load, NODES, 0, 0, tiled=True)
    row = seen[..., :half].sum(axis=0)
    lines = seen[..., half:].reshape(lax.axis_size("near"), -1, rank // nodes, 128).sum(axis=1)
    far = to_each(jnp.concatenate([row.reshape(1, -1), lines.reshape(1, -1)], axis=1), "far")
    row = far[:, :, :columns].sum(axis=0) / replicas
    right = to_each(row, NODES).reshape(rank, 1, half)
    gram = far[:, 0, columns:].reshape(rank, rank)
    flipped = factor_of(0.5 * (gram + gram.T), tiles)
    right, flipped = lax.optimization_barrier((right, flipped))
    other = lax.ppermute(right, "core", SWAP)
    ready = near_half_of(place, flipped, right, deltas, errors)
    return outputs_of(place, flipped, right, other, ready, deltas, errors, momentum)


def solution(mesh):
    torus = Mesh(mesh.devices.reshape(8, 2, 2, 16), ("far", "near", "core", "mdl"))
    in_specs = (P(REP, "mdl", None), P(REP, "mdl", None), P(), P("mdl", REP))
    out_specs = (P(REP, "mdl", None), P("mdl", REP), P("mdl", REP))
    return jax.shard_map(body, mesh=torus, in_specs=in_specs, out_specs=out_specs, check_vma=False)
```

```python
import jax
import jax.numpy as jnp
from jax import lax
from jax.experimental import pallas as pl
from jax.experimental.pallas import tpu as pltpu
from jax.sharding import Mesh
from jax.sharding import PartitionSpec as P

REP = ("far", "near", "core")
PAIR = ("near", "core")
NODES = ("near", "mdl")
SWAP = [(0, 1), (1, 0)]
CHUNKS = 4
BLOCK = 4


highest = lax.Precision.HIGHEST
ANY = pl.BlockSpec(memory_space=pl.ANY)
HBM = pl.BlockSpec(memory_space=pltpu.HBM)
VMEM = pl.BlockSpec(memory_space=pltpu.VMEM)
SMEM = pl.BlockSpec(memory_space=pltpu.SMEM)
SMALL = pltpu.CompilerParams(vmem_limit_bytes=24 << 20)


def held(shape):
    return pltpu.VMEM(shape, jnp.float32)


def near_core(values):
    return pltpu.with_memory_space_constraint(values, pltpu.VMEM)


def far_off(values):
    return pltpu.with_memory_space_constraint(values, pltpu.HBM)


def pieces_of(values, count):
    found = []
    for _ in range(count):
        piece = values.astype(jnp.bfloat16)
        found.append(piece)
        values = values - piece.astype(jnp.float32)
    return found


def dot(a, b, dims):
    return lax.dot_general(a, b, (dims, ((), ())), preferred_element_type=jnp.float32)


def folded(stack, count):
    rows = stack.shape[0] // count
    return sum(stack[i * rows : (i + 1) * rows] for i in reversed(range(count)))


def packed(rows):
    lanes = rows.shape[1] - 128
    count = 128 // lanes
    share = rows.shape[0] // count
    tails = [rows[i * share : (i + 1) * share, 128:] for i in range(count)]
    return rows[:, :128], jnp.concatenate(tails, axis=1)


def unpacked(tiles, lanes):
    count = 128 // lanes
    share = tiles.shape[0] // (count + 1)
    tails = tiles[count * share :]
    tails = [tails[:, i * lanes : (i + 1) * lanes] for i in range(count)]
    return jnp.concatenate([tiles[: count * share], jnp.concatenate(tails, axis=0)], axis=1)


def left_kernel(deltas, errors, starts, out, d_buf, e_buf, s_buf, sems):
    copies = [
        pltpu.make_async_copy(starts, s_buf, sems.at[0]),
        pltpu.make_async_copy(deltas, d_buf, sems.at[1]),
        pltpu.make_async_copy(errors, e_buf, sems.at[2]),
    ]
    for copy in copies:
        copy.start()
    copies[0].wait()
    stack = jnp.concatenate(pieces_of(s_buf[...], 3), axis=0)
    copies[1].wait()
    total = dot(stack, d_buf[0], ((1,), (1,)))
    copies[2].wait()
    total = folded(total + dot(stack, e_buf[0], ((1,), (1,))), 3)
    rank, rows = total.shape
    half = d_buf.shape[2] // 2
    for p in range(2):
        head, tail = packed(total[p * (rank // 2) : (p + 1) * (rank // 2)])
        out[p, : rank // 2] = head
        at = rank // 2 + tail.shape[0]
        out[p, rank // 2 : at] = tail
        for j in range(half // 128):
            cut = slice(p * half + j * 128, p * half + (j + 1) * 128)
            out[p, at + j * rows : at + (j + 1) * rows] = d_buf[0, :, cut].astype(jnp.float32) + e_buf[
                0, :, cut
            ].astype(jnp.float32)


def left_part_of(deltas, errors, starts):
    rows, columns = deltas.shape[1:]
    rank = starts.shape[0]
    size = rank // 2 * rows // 128 + columns // 2 // 128 * rows
    return pl.pallas_call(
        left_kernel,
        out_shape=(
            held((2, size, 128)),
            pltpu.VMEM(deltas.shape, jnp.bfloat16),
            pltpu.VMEM(errors.shape, jnp.bfloat16),
        ),
        in_specs=[HBM, HBM, HBM],
        out_specs=(VMEM, VMEM, VMEM),
        scratch_shapes=[held((rank, columns)), pltpu.SemaphoreType.DMA((3,))],
        compiler_params=SMALL,
        name="left_part",
    )(far_off(deltas), far_off(errors), far_off(starts))


def gram_lines(left, first, count):
    rank = left.shape[0]
    share = 128 // rank
    index = lax.broadcasted_iota(jnp.int32, left.shape, 0)
    nothing = jnp.zeros_like(left)
    lines = None
    for i in range(share):
        own = jnp.concatenate(
            [
                jnp.sum(jnp.where(index == first + share * n + i, left, nothing), axis=0, keepdims=True)
                for n in range(count)
            ],
            axis=0,
        )
        lanes = jnp.concatenate([nothing] * i + [left] + [nothing] * (share - 1 - i), axis=0)
        part = lax.dot_general(
            own, lanes, (((1,), (1,)), ((), ())), precision=highest, preferred_element_type=jnp.float32
        )
        lines = part if lines is None else lines + part
    return lines


def right_kernel(place, halves, merged, out, left):
    rank, rows = left.shape
    columns = out.shape[2] - 128
    chunks = CHUNKS // 2
    width = columns // chunks
    tiles = width // 128
    skip = halves.shape[1]
    whole = jnp.concatenate([unpacked(halves[c] + halves[2 + c], rows - 128) for c in range(2)], axis=0)
    left[...] = whole
    stack = jnp.concatenate(pieces_of(whole, 3), axis=0)
    for j in range(chunks):
        spans = [slice(skip + (j * tiles + t) * rows, skip + (j * tiles + t + 1) * rows) for t in range(tiles)]
        both = jnp.concatenate([merged[0, span] + merged[1, span] for span in spans], axis=1)
        part = None
        for piece in reversed(pieces_of(both, 3)):
            term = dot(stack, piece, ((1,), (0,)))
            part = term if part is None else part + term
        out[:, 0, j * width : (j + 1) * width] = folded(part, 3)
    lines = gram_lines(whole, place[0] // 2 * 4, 2)
    parity = lax.broadcasted_iota(jnp.int32, (rank, lines.shape[1]), 0) % 2
    out[:, 0, columns:] = jnp.where(parity == 0, lines[0:1], lines[1:2])


def right_part_of(place, halves, merged, rank, rows):
    columns = (merged.shape[1] - halves.shape[1]) * 128 // rows
    return pl.pallas_call(
        right_kernel,
        out_shape=(held((rank, 1, columns + 128)), held((rank, rows))),
        in_specs=[SMEM, VMEM, VMEM],
        out_specs=(VMEM, VMEM),
        compiler_params=SMALL,
        name="right_part",
    )(place, near_core(halves), near_core(merged))


def lower_inverse_of(gram):
    rank = gram.shape[0]
    ident = jnp.where(
        lax.broadcasted_iota(jnp.int32, (rank, rank), 0) == lax.broadcasted_iota(jnp.int32, (rank, rank), 1), 1.0, 0.0
    )
    table = jnp.concatenate([gram, ident], axis=1)
    index = lax.broadcasted_iota(jnp.int32, table.shape, 0)
    for k in range(0, rank, BLOCK):
        cols = [jnp.broadcast_to(table[:, k + j : k + j + 1], table.shape) for j in range(BLOCK)]
        for j in range(BLOCK):
            at = k + j
            scale = 1.0 / cols[j][at : at + 1]
            ratio = jnp.where(index > at, cols[j] * scale, 0.0)
            for n in range(j + 1, BLOCK):
                cols[n] = cols[n] - ratio * cols[n][at : at + 1]
            line = table[at : at + 1]
            table = jnp.where(index == at, line * jnp.sqrt(scale), table - ratio * line)
    lane = lax.broadcasted_iota(jnp.int32, table.shape, 1)
    return jnp.where(lane < rank, pltpu.roll(table, rank, 1), table)


def factor_kernel(gram, left, out):
    rank = gram.shape[0]
    whole = left[...]
    inverse = lower_inverse_of(gram[...])
    basis = lax.dot_general(
        inverse[:, :rank], whole, (((1,), (0,)), ((), ())), precision=highest, preferred_element_type=jnp.float32
    )
    twice = lax.dot_general(
        basis, inverse, (((0,), (0,)), ((), ())), precision=highest, preferred_element_type=jnp.float32
    )
    out[...] = jnp.concatenate(pieces_of(twice, 2), axis=1)


def factor_of(gram, left):
    return pl.pallas_call(
        factor_kernel,
        out_shape=pltpu.VMEM((left.shape[1], 4 * gram.shape[0]), jnp.bfloat16),
        in_specs=[VMEM, VMEM],
        out_specs=VMEM,
        compiler_params=SMALL,
        cost_estimate=pl.CostEstimate(flops=40_000_000, transcendentals=0, bytes_accessed=200_000),
        name="factor",
    )(near_core(gram), near_core(left))


def product(flipped, right):
    big, small = pieces_of(right, 2)
    return dot(flipped, jnp.concatenate([big, small, big, small], axis=0), ((1,), (0,)))


def residue(flipped, right, deltas, errors, base, j, width):
    approx = product(flipped[...], right[:, 0, j * width : (j + 1) * width])
    cut = pl.ds(pl.multiple_of(base + j * width, 128), width)
    merged = deltas[0, :, cut].astype(jnp.float32) + errors[0, :, cut].astype(jnp.float32)
    return (merged - approx).astype(jnp.bfloat16)


def near_kernel(place, flipped, right, deltas, errors, out):
    half = right.shape[2]
    width = half // (CHUNKS // 2)
    base = place[0] % 2 * half
    for j in range(CHUNKS // 2):
        out[:, j * width : (j + 1) * width] = residue(flipped, right, deltas, errors, base, j, width)


def near_half_of(place, flipped, right, deltas, errors):
    return pl.pallas_call(
        near_kernel,
        out_shape=pltpu.VMEM((deltas.shape[1], right.shape[2]), jnp.bfloat16),
        in_specs=[SMEM, VMEM, VMEM, VMEM, VMEM],
        out_specs=VMEM,
        compiler_params=SMALL,
        cost_estimate=pl.CostEstimate(flops=40_000_000, transcendentals=0, bytes_accessed=2_000_000),
        name="near_half",
    )(place, near_core(flipped), near_core(right), near_core(deltas), near_core(errors))


def out_kernel(place, flipped, right, other, ready, deltas, errors, momentum, new_errors, new_momentum, outer_step, buf, fresh, step, sems):
    half = right.shape[2]
    owned = momentum.shape[1]
    each = half // owned
    core = place[0] % 2
    own = pl.ds(pl.multiple_of(core * half, 128), half)
    copies = [pltpu.make_async_copy(ready, new_errors.at[0, :, own], sems.at[0])]
    copies[0].start()
    first = place[0] % each * owned
    base = pl.multiple_of(jnp.minimum(first // 128, half // 128 - 2) * 128, 128)
    cut = pl.ds(base, 256)
    window = jnp.where(place[0] // each == core, right[:, 0, cut], other[:, 0, cut])
    window = pltpu.roll(window, lax.rem(256 - (first - base), 256), 1)[:, :128]
    mine = product(flipped[...], window)[:, :owned]
    fresh[...] = 0.9 * momentum[...] + mine
    step[...] = 0.7 * (mine + 0.9 * fresh[...])
    copies.append(pltpu.make_async_copy(fresh, new_momentum, sems.at[1]))
    copies.append(pltpu.make_async_copy(step, outer_step, sems.at[2]))
    for copy in copies[1:]:
        copy.start()
    width = half // (CHUNKS // 2)
    base = (1 - core) * half
    for j in range(CHUNKS // 2):
        cut = slice(j * width, (j + 1) * width)
        buf[:, cut] = residue(flipped, other, deltas, errors, base, j, width)
        there = pl.ds(pl.multiple_of(base + j * width, 128), width)
        copy = pltpu.make_async_copy(buf.at[:, pl.ds(j * width, width)], new_errors.at[0, :, there], sems.at[3 + j])
        copy.start()
        copies.append(copy)
    for copy in copies:
        copy.wait()


def outputs_of(place, flipped, right, other, ready, deltas, errors, momentum):
    f32 = jnp.float32
    return pl.pallas_call(
        out_kernel,
        out_shape=(
            jax.ShapeDtypeStruct(deltas.shape, jnp.bfloat16),
            jax.ShapeDtypeStruct(momentum.shape, f32),
            jax.ShapeDtypeStruct(momentum.shape, f32),
        ),
        in_specs=[SMEM] + [VMEM] * 7,
        out_specs=(HBM, HBM, HBM),
        scratch_shapes=[
            pltpu.VMEM(ready.shape, jnp.bfloat16),
            held(momentum.shape),
            held(momentum.shape),
            pltpu.SemaphoreType.DMA((3 + CHUNKS // 2,)),
        ],
        compiler_params=SMALL,
        name="outputs",
    )(place, *(near_core(a) for a in (flipped, right, other, ready, deltas, errors, momentum)))


def to_each(shard, axes):
    count = lax.axis_size(axes)
    return lax.all_to_all(
        jnp.broadcast_to(shard[None], (count, *shard.shape)), axes, 0, 0, tiled=True
    )


def body(deltas, errors, starts, momentum):
    replicas = lax.axis_size(REP)
    rank = starts.shape[1]
    columns = deltas.shape[2]
    place = lax.axis_index(REP)[None]
    load, deltas, errors = left_part_of(deltas, errors, starts.T)
    load, place = lax.optimization_barrier((load, place))
    merged = lax.all_to_all(load, "core", 0, 0, tiled=True)
    size = rank // 2 * deltas.shape[1] // 128
    own = to_each(merged[:, :size].sum(axis=0), "far").sum(axis=0) / replicas
    load, left = right_part_of(place, to_each(own, PAIR), merged, rank, deltas.shape[1])
    half = columns // 2
    nodes = lax.axis_size(NODES)
    load = load.reshape(nodes, rank // nodes, 1, -1)
    seen = lax.all_to_all(load, NODES, 0, 0, tiled=True)
    row = seen[..., :half].sum(axis=0)
    lines = seen[..., half:].reshape(lax.axis_size("near"), -1, rank // nodes, 128).sum(axis=1)
    far = to_each(jnp.concatenate([row.reshape(1, -1), lines.reshape(1, -1)], axis=1), "far")
    row = far[:, :, :columns].sum(axis=0) / replicas
    right = to_each(row, NODES).reshape(rank, 1, half)
    gram = far[:, 0, columns:].reshape(rank, rank)
    flipped = factor_of(0.5 * (gram + gram.T), left)
    right, flipped = lax.optimization_barrier((right, flipped))
    other = lax.ppermute(right, "core", SWAP)
    ready = near_half_of(place, flipped, right, deltas, errors)
    return outputs_of(place, flipped, right, other, ready, deltas, errors, momentum)


def solution(mesh):
    torus = Mesh(mesh.devices.reshape(8, 2, 2, 16), ("far", "near", "core", "mdl"))
    in_specs = (P(REP, "mdl", None), P(REP, "mdl", None), P(), P("mdl", REP))
    out_specs = (P(REP, "mdl", None), P("mdl", REP), P("mdl", REP))
    return jax.shard_map(body, mesh=torus, in_specs=in_specs, out_specs=out_specs, check_vma=False)
```

```python
import jax
import jax.numpy as jnp
from jax import lax
from jax.experimental import pallas as pl
from jax.experimental.pallas import tpu as pltpu
from jax.sharding import Mesh
from jax.sharding import PartitionSpec as P

REP = ("far", "near", "core")
PAIR = ("near", "core")
NODES = ("near", "mdl")
SWAP = [(0, 1), (1, 0)]
CHUNKS = 4
BLOCK = 4


highest = lax.Precision.HIGHEST
ANY = pl.BlockSpec(memory_space=pl.ANY)
HBM = pl.BlockSpec(memory_space=pltpu.HBM)
VMEM = pl.BlockSpec(memory_space=pltpu.VMEM)
SMEM = pl.BlockSpec(memory_space=pltpu.SMEM)
SMALL = pltpu.CompilerParams(vmem_limit_bytes=24 << 20)


def held(shape):
    return pltpu.VMEM(shape, jnp.float32)


def near_core(values):
    return pltpu.with_memory_space_constraint(values, pltpu.VMEM)


def far_off(values):
    return pltpu.with_memory_space_constraint(values, pltpu.HBM)


def pieces_of(values, count):
    found = []
    for _ in range(count):
        piece = values.astype(jnp.bfloat16)
        found.append(piece)
        values = values - piece.astype(jnp.float32)
    return found


def dot(a, b, dims):
    return lax.dot_general(a, b, (dims, ((), ())), preferred_element_type=jnp.float32)


def folded(stack, count):
    rows = stack.shape[0] // count
    return sum(stack[i * rows : (i + 1) * rows] for i in reversed(range(count)))


def packed(rows):
    lanes = rows.shape[1] - 128
    count = 128 // lanes
    share = rows.shape[0] // count
    tails = [rows[i * share : (i + 1) * share, 128:] for i in range(count)]
    return rows[:, :128], jnp.concatenate(tails, axis=1)


def unpacked(tiles, lanes):
    count = 128 // lanes
    share = tiles.shape[0] // (count + 1)
    tails = tiles[count * share :]
    tails = [tails[:, i * lanes : (i + 1) * lanes] for i in range(count)]
    return jnp.concatenate([tiles[: count * share], jnp.concatenate(tails, axis=0)], axis=1)


def left_kernel(deltas, errors, starts, out, d_buf, e_buf, s_buf, sems):
    copies = [
        pltpu.make_async_copy(starts, s_buf, sems.at[0]),
        pltpu.make_async_copy(deltas, d_buf, sems.at[1]),
        pltpu.make_async_copy(errors, e_buf, sems.at[2]),
    ]
    for copy in copies:
        copy.start()
    copies[0].wait()
    stack = jnp.concatenate(pieces_of(s_buf[...], 3), axis=0)
    copies[1].wait()
    total = dot(stack, d_buf[0], ((1,), (1,)))
    copies[2].wait()
    total = folded(total + dot(stack, e_buf[0], ((1,), (1,))), 3)
    rank, rows = total.shape
    half = d_buf.shape[2] // 2
    for p in range(2):
        head, tail = packed(total[p * (rank // 2) : (p + 1) * (rank // 2)])
        out[p, : rank // 2] = head
        at = rank // 2 + tail.shape[0]
        out[p, rank // 2 : at] = tail
        for j in range(half // 128):
            cut = slice(p * half + j * 128, p * half + (j + 1) * 128)
            out[p, at + j * rows : at + (j + 1) * rows] = d_buf[0, :, cut].astype(jnp.float32) + e_buf[
                0, :, cut
            ].astype(jnp.float32)


def left_part_of(deltas, errors, starts):
    rows, columns = deltas.shape[1:]
    rank = starts.shape[0]
    size = rank // 2 * rows // 128 + columns // 2 // 128 * rows
    return pl.pallas_call(
        left_kernel,
        out_shape=(
            held((2, size, 128)),
            pltpu.VMEM(deltas.shape, jnp.bfloat16),
            pltpu.VMEM(errors.shape, jnp.bfloat16),
        ),
        in_specs=[HBM, HBM, HBM],
        out_specs=(VMEM, VMEM, VMEM),
        scratch_shapes=[held((rank, columns)), pltpu.SemaphoreType.DMA((3,))],
        compiler_params=SMALL,
        name="left_part",
    )(far_off(deltas), far_off(errors), far_off(starts))


def gram_lines(left, first, count):
    index = lax.broadcasted_iota(jnp.int32, left.shape, 0)
    own = [jnp.sum(jnp.where(index == first + i, left, 0.0), axis=0, keepdims=True) for i in range(count)]
    return lax.dot_general(
        jnp.concatenate(own, axis=0), left, (((1,), (1,)), ((), ())), precision=highest, preferred_element_type=jnp.float32
    )


def right_kernel(place, halves, merged, out, left):
    rank, rows = left.shape
    share = out.shape[1]
    groups = rank // share
    width = out.shape[2] - rank
    tiles = width // 128
    skip = halves.shape[1]
    whole = jnp.concatenate([unpacked(halves[c] + halves[2 + c], rows - 128) for c in range(2)], axis=0)
    left[...] = whole
    stack = jnp.concatenate(pieces_of(whole, 3), axis=0)
    for j in range(out.shape[0] // groups):
        spans = [slice(skip + (j * tiles + t) * rows, skip + (j * tiles + t + 1) * rows) for t in range(tiles)]
        both = jnp.concatenate([merged[0, span] + merged[1, span] for span in spans], axis=1)
        part = None
        for piece in reversed(pieces_of(both, 3)):
            term = dot(stack, piece, ((1,), (0,)))
            part = term if part is None else part + term
        part = folded(part, 3)
        for g in range(groups):
            out[j * groups + g, :, :width] = part[g * share : (g + 1) * share]
    lines = gram_lines(whole, place[0] // 2 * share, share)
    for p in range(out.shape[0]):
        out[p, :, width:] = lines


def right_part_of(place, halves, merged, rank, rows):
    width = (merged.shape[1] - halves.shape[1]) * 128 // rows // 2
    share = rank * 2 // lax.axis_size(NODES)
    return pl.pallas_call(
        right_kernel,
        out_shape=(held((rank * 2 // share, share, width + rank)), held((rank, rows))),
        in_specs=[SMEM, VMEM, VMEM],
        out_specs=(VMEM, VMEM),
        compiler_params=SMALL,
        name="right_part",
    )(place, near_core(halves), near_core(merged))


def lower_inverse_of(gram):
    rank = gram.shape[0]
    ident = jnp.where(
        lax.broadcasted_iota(jnp.int32, (rank, rank), 0) == lax.broadcasted_iota(jnp.int32, (rank, rank), 1), 1.0, 0.0
    )
    table = jnp.concatenate([gram, ident], axis=1)
    index = lax.broadcasted_iota(jnp.int32, table.shape, 0)
    for k in range(0, rank, BLOCK):
        cols = [jnp.broadcast_to(table[:, k + j : k + j + 1], table.shape) for j in range(BLOCK)]
        for j in range(BLOCK):
            at = k + j
            scale = 1.0 / cols[j][at : at + 1]
            ratio = jnp.where(index > at, cols[j] * scale, 0.0)
            for n in range(j + 1, BLOCK):
                cols[n] = cols[n] - ratio * cols[n][at : at + 1]
            line = table[at : at + 1]
            table = jnp.where(index == at, line * jnp.sqrt(scale), table - ratio * line)
    lane = lax.broadcasted_iota(jnp.int32, table.shape, 1)
    return jnp.where(lane < rank, pltpu.roll(table, rank, 1), table)


def factor_kernel(gram, left, out):
    rank = gram.shape[0]
    whole = left[...]
    inverse = lower_inverse_of(gram[...])
    basis = lax.dot_general(
        inverse[:, :rank], whole, (((1,), (0,)), ((), ())), precision=highest, preferred_element_type=jnp.float32
    )
    twice = lax.dot_general(
        basis, inverse, (((0,), (0,)), ((), ())), precision=highest, preferred_element_type=jnp.float32
    )
    out[...] = jnp.concatenate(pieces_of(twice, 2), axis=1)


def factor_of(gram, left):
    return pl.pallas_call(
        factor_kernel,
        out_shape=pltpu.VMEM((left.shape[1], 4 * gram.shape[0]), jnp.bfloat16),
        in_specs=[VMEM, VMEM],
        out_specs=VMEM,
        compiler_params=SMALL,
        cost_estimate=pl.CostEstimate(flops=40_000_000, transcendentals=0, bytes_accessed=200_000),
        name="factor",
    )(near_core(gram), near_core(left))


def product(flipped, right):
    big, small = pieces_of(right, 2)
    return dot(flipped, jnp.concatenate([big, small, big, small], axis=0), ((1,), (0,)))


def flatten(right, flat):
    share, width = right.shape[1:]
    groups = flat.shape[0] // share
    for j in range(right.shape[0] // groups):
        for g in range(groups):
            flat[g * share : (g + 1) * share, j * width : (j + 1) * width] = right[j * groups + g]


def residue(flipped, flat, deltas, errors, base, j, width):
    approx = product(flipped[...], flat[:, j * width : (j + 1) * width])
    cut = pl.ds(pl.multiple_of(base + j * width, 128), width)
    merged = deltas[0, :, cut].astype(jnp.float32) + errors[0, :, cut].astype(jnp.float32)
    return (merged - approx).astype(jnp.bfloat16)


def near_kernel(place, flipped, right, deltas, errors, out, flat):
    flatten(right, flat)
    half = flat.shape[1]
    width = half // (CHUNKS // 2)
    base = place[0] % 2 * half
    for j in range(CHUNKS // 2):
        out[:, j * width : (j + 1) * width] = residue(flipped, flat, deltas, errors, base, j, width)


def near_half_of(place, flipped, right, deltas, errors):
    rows, columns = deltas.shape[1:]
    rank = right.size * 2 // columns
    return pl.pallas_call(
        near_kernel,
        out_shape=(pltpu.VMEM((rows, columns // 2), jnp.bfloat16), held((rank, columns // 2))),
        in_specs=[SMEM, VMEM, VMEM, VMEM, VMEM],
        out_specs=(VMEM, VMEM),
        compiler_params=SMALL,
        cost_estimate=pl.CostEstimate(flops=40_000_000, transcendentals=0, bytes_accessed=2_000_000),
        name="near_half",
    )(place, near_core(flipped), near_core(right), near_core(deltas), near_core(errors))


def out_kernel(place, flipped, right, other, ready, deltas, errors, momentum, new_errors, new_momentum, outer_step, flat, buf, fresh, step, sems):
    half = right.shape[1]
    owned = momentum.shape[1]
    each = half // owned
    core = place[0] % 2
    own = pl.ds(pl.multiple_of(core * half, 128), half)
    copies = [pltpu.make_async_copy(ready, new_errors.at[0, :, own], sems.at[0])]
    copies[0].start()
    flatten(other, flat)
    width = half // (CHUNKS // 2)
    far = (1 - core) * half
    for j in range(CHUNKS // 2):
        cut = slice(j * width, (j + 1) * width)
        buf[:, cut] = residue(flipped, flat, deltas, errors, far, j, width)
        there = pl.ds(pl.multiple_of(far + j * width, 128), width)
        copy = pltpu.make_async_copy(buf.at[:, pl.ds(j * width, width)], new_errors.at[0, :, there], sems.at[3 + j])
        copy.start()
        copies.append(copy)
        if j == 0:
            first = place[0] % each * owned
            base = pl.multiple_of(jnp.minimum(first // 128, half // 128 - 2) * 128, 128)
            cut = pl.ds(base, 256)
            window = jnp.where(place[0] // each == core, right[:, cut], flat[:, cut])
            window = pltpu.roll(window, lax.rem(256 - (first - base), 256), 1)[:, :128]
            mine = product(flipped[...], window)[:, :owned]
            fresh[...] = 0.9 * momentum[...] + mine
            step[...] = 0.7 * (mine + 0.9 * fresh[...])
            for k, (source, target) in enumerate(((fresh, new_momentum), (step, outer_step))):
                copy = pltpu.make_async_copy(source, target, sems.at[1 + k])
                copy.start()
                copies.append(copy)
    for copy in copies:
        copy.wait()


def outputs_of(place, flipped, right, other, ready, deltas, errors, momentum):
    f32 = jnp.float32
    return pl.pallas_call(
        out_kernel,
        out_shape=(
            jax.ShapeDtypeStruct(deltas.shape, jnp.bfloat16),
            jax.ShapeDtypeStruct(momentum.shape, f32),
            jax.ShapeDtypeStruct(momentum.shape, f32),
        ),
        in_specs=[SMEM] + [VMEM] * 7,
        out_specs=(HBM, HBM, HBM),
        scratch_shapes=[
            held(right.shape),
            pltpu.VMEM(ready.shape, jnp.bfloat16),
            held(momentum.shape),
            held(momentum.shape),
            pltpu.SemaphoreType.DMA((3 + CHUNKS // 2,)),
        ],
        compiler_params=SMALL,
        name="outputs",
    )(place, *(near_core(a) for a in (flipped, right, other, ready, deltas, errors, momentum)))


def to_each(shard, axes):
    count = lax.axis_size(axes)
    return lax.all_to_all(
        jnp.broadcast_to(shard[None], (count, *shard.shape)), axes, 0, 0, tiled=True
    )


def body(deltas, errors, starts, momentum):
    replicas = lax.axis_size(REP)
    rank = starts.shape[1]
    place = lax.axis_index(REP)[None]
    load, deltas, errors = left_part_of(deltas, errors, starts.T)
    load, place = lax.optimization_barrier((load, place))
    merged = lax.all_to_all(load, "core", 0, 0, tiled=True)
    size = rank // 2 * deltas.shape[1] // 128
    own = to_each(merged[:, :size].sum(axis=0), "far").sum(axis=0) / replicas
    load, left = right_part_of(place, to_each(own, PAIR), merged, rank, deltas.shape[1])
    nodes = lax.axis_size(NODES)
    width = load.shape[2] - rank
    seen = lax.all_to_all(load, NODES, 0, 0, tiled=True)
    lines = seen[:, :, width:].reshape(lax.axis_size("near"), -1, *seen.shape[1:2], rank).sum(axis=1)
    far = to_each(jnp.concatenate([seen[:, :, :width].sum(axis=0), *lines], axis=1), "far")
    part = far[:, :, :width].sum(axis=0) / replicas
    right = to_each(part, NODES).reshape(nodes, -1, width)
    gram = jnp.moveaxis(far[:, :, width:].reshape(*far.shape[:2], -1, rank), 2, 1).reshape(rank, rank)
    flipped = factor_of(0.5 * (gram + gram.T), left)
    right, flipped = lax.optimization_barrier((right, flipped))
    other = lax.ppermute(right, "core", SWAP)
    ready, flat = near_half_of(place, flipped, right, deltas, errors)
    return outputs_of(place, flipped, flat, other, ready, deltas, errors, momentum)


def solution(mesh):
    torus = Mesh(mesh.devices.reshape(8, 2, 2, 16), ("far", "near", "core", "mdl"))
    in_specs = (P(REP, "mdl", None), P(REP, "mdl", None), P(), P("mdl", REP))
    out_specs = (P(REP, "mdl", None), P("mdl", REP), P("mdl", REP))
    return jax.shard_map(body, mesh=torus, in_specs=in_specs, out_specs=out_specs, check_vma=False)
```

```python
import jax
import jax.numpy as jnp
from jax import lax
from jax.experimental import pallas as pl
from jax.experimental.pallas import tpu as pltpu
from jax.sharding import Mesh
from jax.sharding import PartitionSpec as P

REP = ("far", "near", "core")
PAIR = ("near", "core")
NODES = ("near", "mdl")
SWAP = [(0, 1), (1, 0)]
CHUNKS = 4
BLOCK = 16


highest = lax.Precision.HIGHEST
ANY = pl.BlockSpec(memory_space=pl.ANY)
HBM = pl.BlockSpec(memory_space=pltpu.HBM)
VMEM = pl.BlockSpec(memory_space=pltpu.VMEM)
SMEM = pl.BlockSpec(memory_space=pltpu.SMEM)
SMALL = pltpu.CompilerParams(vmem_limit_bytes=24 << 20)


def held(shape):
    return pltpu.VMEM(shape, jnp.float32)


def near_core(values):
    return pltpu.with_memory_space_constraint(values, pltpu.VMEM)


def far_off(values):
    return pltpu.with_memory_space_constraint(values, pltpu.HBM)


def pieces_of(values, count):
    found = []
    for _ in range(count):
        piece = values.astype(jnp.bfloat16)
        found.append(piece)
        values = values - piece.astype(jnp.float32)
    return found


def dot(a, b, dims):
    return lax.dot_general(a, b, (dims, ((), ())), preferred_element_type=jnp.float32)


def folded(stack, count):
    rows = stack.shape[0] // count
    return sum(stack[i * rows : (i + 1) * rows] for i in reversed(range(count)))


def packed(rows):
    lanes = rows.shape[1] - 128
    count = 128 // lanes
    share = rows.shape[0] // count
    tails = [rows[i * share : (i + 1) * share, 128:] for i in range(count)]
    return rows[:, :128], jnp.concatenate(tails, axis=1)


def unpacked(tiles, lanes):
    count = 128 // lanes
    share = tiles.shape[0] // (count + 1)
    tails = tiles[count * share :]
    tails = [tails[:, i * lanes : (i + 1) * lanes] for i in range(count)]
    return jnp.concatenate([tiles[: count * share], jnp.concatenate(tails, axis=0)], axis=1)


def left_kernel(deltas, errors, starts, out, d_buf, e_buf, s_buf, sems):
    copies = [
        pltpu.make_async_copy(starts, s_buf, sems.at[0]),
        pltpu.make_async_copy(deltas, d_buf, sems.at[1]),
        pltpu.make_async_copy(errors, e_buf, sems.at[2]),
    ]
    for copy in copies:
        copy.start()
    copies[0].wait()
    stack = jnp.concatenate(pieces_of(s_buf[...], 3), axis=0)
    copies[1].wait()
    total = dot(stack, d_buf[0], ((1,), (1,)))
    copies[2].wait()
    total = folded(total + dot(stack, e_buf[0], ((1,), (1,))), 3)
    rank, rows = total.shape
    half = d_buf.shape[2] // 2
    for p in range(2):
        head, tail = packed(total[p * (rank // 2) : (p + 1) * (rank // 2)])
        out[p, : rank // 2] = head
        at = rank // 2 + tail.shape[0]
        out[p, rank // 2 : at] = tail
        for j in range(half // 128):
            cut = slice(p * half + j * 128, p * half + (j + 1) * 128)
            out[p, at + j * rows : at + (j + 1) * rows] = d_buf[0, :, cut].astype(jnp.float32) + e_buf[
                0, :, cut
            ].astype(jnp.float32)


def left_part_of(deltas, errors, starts):
    rows, columns = deltas.shape[1:]
    rank = starts.shape[0]
    size = rank // 2 * rows // 128 + columns // 2 // 128 * rows
    return pl.pallas_call(
        left_kernel,
        out_shape=(
            held((2, size, 128)),
            pltpu.VMEM(deltas.shape, jnp.bfloat16),
            pltpu.VMEM(errors.shape, jnp.bfloat16),
        ),
        in_specs=[HBM, HBM, HBM],
        out_specs=(VMEM, VMEM, VMEM),
        scratch_shapes=[held((rank, columns)), pltpu.SemaphoreType.DMA((3,))],
        compiler_params=SMALL,
        name="left_part",
    )(far_off(deltas), far_off(errors), far_off(starts))


def right_kernel(halves, merged, out, left):
    rank, rows = left.shape
    share = out.shape[1]
    groups = rank // share
    width = out.shape[2] - rank
    tiles = width // 128
    skip = halves.shape[1]
    whole = jnp.concatenate([unpacked(halves[c] + halves[2 + c], rows - 128) for c in range(2)], axis=0)
    left[...] = whole
    stack = jnp.concatenate(pieces_of(whole, 3), axis=0)
    for j in range(out.shape[0] // groups):
        spans = [slice(skip + (j * tiles + t) * rows, skip + (j * tiles + t + 1) * rows) for t in range(tiles)]
        both = jnp.concatenate([merged[0, span] + merged[1, span] for span in spans], axis=1)
        part = None
        for piece in reversed(pieces_of(both, 3)):
            term = dot(stack, piece, ((1,), (0,)))
            part = term if part is None else part + term
        part = folded(part, 3)
        for g in range(groups):
            out[j * groups + g, :, :width] = part[g * share : (g + 1) * share]
    gram = lax.dot_general(
        whole, whole, (((1,), (1,)), ((), ())), precision=highest, preferred_element_type=jnp.float32
    )
    lines = rank // out.shape[0]
    for p in range(out.shape[0]):
        out[p, :lines, width:] = gram[p * lines : (p + 1) * lines]
        out[p, lines:, width:] = jnp.zeros((share - lines, rank), jnp.float32)


def right_part_of(halves, merged, rank, rows):
    width = (merged.shape[1] - halves.shape[1]) * 128 // rows // 2
    share = rank * 2 // lax.axis_size(NODES)
    return pl.pallas_call(
        right_kernel,
        out_shape=(held((rank * 2 // share, share, width + rank)), held((rank, rows))),
        in_specs=[VMEM, VMEM],
        out_specs=(VMEM, VMEM),
        compiler_params=SMALL,
        name="right_part",
    )(near_core(halves), near_core(merged))


def lower_inverse_of(gram):
    rank = gram.shape[0]
    ident = jnp.where(
        lax.broadcasted_iota(jnp.int32, (rank, rank), 0) == lax.broadcasted_iota(jnp.int32, (rank, rank), 1), 1.0, 0.0
    )
    table = jnp.concatenate([gram, ident], axis=1)
    index = lax.broadcasted_iota(jnp.int32, table.shape, 0)
    for k in range(0, rank, BLOCK):
        cols = [jnp.broadcast_to(table[:, k + j : k + j + 1], table.shape) for j in range(BLOCK)]
        for j in range(BLOCK):
            at = k + j
            scale = 1.0 / cols[j][at : at + 1]
            ratio = jnp.where(index > at, cols[j] * scale, 0.0)
            for n in range(j + 1, BLOCK):
                cols[n] = cols[n] - ratio * cols[n][at : at + 1]
            line = table[at : at + 1]
            table = jnp.where(index == at, line * jnp.sqrt(scale), table - ratio * line)
    lane = lax.broadcasted_iota(jnp.int32, table.shape, 1)
    return jnp.where(lane < rank, pltpu.roll(table, rank, 1), table)


def factor_kernel(right, left, out, gram):
    rank = left.shape[0]
    width = right.shape[2] - rank
    lines = rank // right.shape[0]
    for p in range(right.shape[0]):
        gram[p * lines : (p + 1) * lines] = right[p, :lines, width:]
    table = gram[...]
    inverse = lower_inverse_of(0.5 * (table + table.T))
    basis = lax.dot_general(
        inverse[:, :rank], left[...], (((1,), (0,)), ((), ())), precision=highest, preferred_element_type=jnp.float32
    )
    twice = lax.dot_general(
        basis, inverse, (((0,), (0,)), ((), ())), precision=highest, preferred_element_type=jnp.float32
    )
    out[...] = jnp.concatenate(pieces_of(twice, 2), axis=1)


def factor_of(right, left):
    rank, rows = left.shape
    return pl.pallas_call(
        factor_kernel,
        out_shape=pltpu.VMEM((rows, 4 * rank), jnp.bfloat16),
        in_specs=[VMEM, VMEM],
        out_specs=VMEM,
        scratch_shapes=[held((rank, rank))],
        compiler_params=SMALL,
        cost_estimate=pl.CostEstimate(flops=40_000_000, transcendentals=0, bytes_accessed=200_000),
        name="factor",
    )(near_core(right), near_core(left))


def product(flipped, right):
    big, small = pieces_of(right, 2)
    return dot(flipped, jnp.concatenate([big, small, big, small], axis=0), ((1,), (0,)))


def flatten(right, flat):
    share = right.shape[1]
    groups = flat.shape[0] // share
    blocks = right.shape[0] // groups
    width = flat.shape[1] // blocks
    for j in range(blocks):
        for g in range(groups):
            flat[g * share : (g + 1) * share, j * width : (j + 1) * width] = right[j * groups + g, :, :width]


def residue(flipped, flat, deltas, errors, base, j, width):
    approx = product(flipped[...], flat[:, j * width : (j + 1) * width])
    cut = pl.ds(pl.multiple_of(base + j * width, 128), width)
    merged = deltas[0, :, cut].astype(jnp.float32) + errors[0, :, cut].astype(jnp.float32)
    return (merged - approx).astype(jnp.bfloat16)


def near_kernel(place, flipped, right, deltas, errors, out, flat):
    flatten(right, flat)
    half = flat.shape[1]
    width = half // (CHUNKS // 2)
    base = place[0] % 2 * half
    for j in range(CHUNKS // 2):
        out[:, j * width : (j + 1) * width] = residue(flipped, flat, deltas, errors, base, j, width)


def near_half_of(place, flipped, right, deltas, errors):
    rows, columns = deltas.shape[1:]
    rank = flipped.shape[1] // 4
    return pl.pallas_call(
        near_kernel,
        out_shape=(pltpu.VMEM((rows, columns // 2), jnp.bfloat16), held((rank, columns // 2))),
        in_specs=[SMEM, VMEM, VMEM, VMEM, VMEM],
        out_specs=(VMEM, VMEM),
        compiler_params=SMALL,
        cost_estimate=pl.CostEstimate(flops=40_000_000, transcendentals=0, bytes_accessed=2_000_000),
        name="near_half",
    )(place, near_core(flipped), near_core(right), near_core(deltas), near_core(errors))


def out_kernel(place, flipped, right, other, ready, deltas, errors, momentum, new_errors, new_momentum, outer_step, flat, buf, fresh, step, sems):
    half = right.shape[1]
    owned = momentum.shape[1]
    each = half // owned
    core = place[0] % 2
    own = pl.ds(pl.multiple_of(core * half, 128), half)
    copies = [pltpu.make_async_copy(ready, new_errors.at[0, :, own], sems.at[0])]
    copies[0].start()
    flatten(other, flat)
    width = half // (CHUNKS // 2)
    far = (1 - core) * half
    for j in range(CHUNKS // 2):
        cut = slice(j * width, (j + 1) * width)
        buf[:, cut] = residue(flipped, flat, deltas, errors, far, j, width)
        there = pl.ds(pl.multiple_of(far + j * width, 128), width)
        copy = pltpu.make_async_copy(buf.at[:, pl.ds(j * width, width)], new_errors.at[0, :, there], sems.at[3 + j])
        copy.start()
        copies.append(copy)
        if j == 0:
            first = place[0] % each * owned
            base = pl.multiple_of(jnp.minimum(first // 128, half // 128 - 2) * 128, 128)
            cut = pl.ds(base, 256)
            window = jnp.where(place[0] // each == core, right[:, cut], flat[:, cut])
            window = pltpu.roll(window, lax.rem(256 - (first - base), 256), 1)[:, :128]
            mine = product(flipped[...], window)[:, :owned]
            fresh[...] = 0.9 * momentum[...] + mine
            step[...] = 0.7 * (mine + 0.9 * fresh[...])
            for k, (source, target) in enumerate(((fresh, new_momentum), (step, outer_step))):
                copy = pltpu.make_async_copy(source, target, sems.at[1 + k])
                copy.start()
                copies.append(copy)
    for copy in copies:
        copy.wait()


def outputs_of(place, flipped, right, other, ready, deltas, errors, momentum):
    f32 = jnp.float32
    return pl.pallas_call(
        out_kernel,
        out_shape=(
            jax.ShapeDtypeStruct(deltas.shape, jnp.bfloat16),
            jax.ShapeDtypeStruct(momentum.shape, f32),
            jax.ShapeDtypeStruct(momentum.shape, f32),
        ),
        in_specs=[SMEM] + [VMEM] * 7,
        out_specs=(HBM, HBM, HBM),
        scratch_shapes=[
            held(right.shape),
            pltpu.VMEM(ready.shape, jnp.bfloat16),
            held(momentum.shape),
            held(momentum.shape),
            pltpu.SemaphoreType.DMA((3 + CHUNKS // 2,)),
        ],
        compiler_params=SMALL,
        name="outputs",
    )(place, *(near_core(a) for a in (flipped, right, other, ready, deltas, errors, momentum)))


def to_each(shard, axes):
    count = lax.axis_size(axes)
    return lax.all_to_all(
        jnp.broadcast_to(shard[None], (count, *shard.shape)), axes, 0, 0, tiled=True
    )


def body(deltas, errors, starts, momentum):
    replicas = lax.axis_size(REP)
    rank = starts.shape[1]
    place = lax.axis_index(REP)[None]
    load, deltas, errors = left_part_of(deltas, errors, starts.T)
    load, place = lax.optimization_barrier((load, place))
    merged = lax.all_to_all(load, "core", 0, 0, tiled=True)
    size = rank // 2 * deltas.shape[1] // 128
    own = to_each(merged[:, :size].sum(axis=0), "far").sum(axis=0) / replicas
    load, left = right_part_of(to_each(own, PAIR), merged, rank, deltas.shape[1])
    nodes = lax.axis_size(NODES)
    width = load.shape[2] - rank
    total = lax.all_to_all(load, NODES, 0, 0, tiled=True).sum(axis=0)
    part, gram = lax.optimization_barrier((total[:, :width], total[:, width:] / lax.axis_size("near")))
    part = to_each(part, "far").sum(axis=0) / replicas
    right = to_each(jnp.concatenate([part, gram], axis=1), NODES).reshape(nodes, *total.shape)
    flipped = factor_of(right, left)
    other = lax.ppermute(right, "core", SWAP)
    ready, flat = near_half_of(place, flipped, right, deltas, errors)
    return outputs_of(place, flipped, flat, other, ready, deltas, errors, momentum)


def solution(mesh):
    torus = Mesh(mesh.devices.reshape(8, 2, 2, 16), ("far", "near", "core", "mdl"))
    in_specs = (P(REP, "mdl", None), P(REP, "mdl", None), P(), P("mdl", REP))
    out_specs = (P(REP, "mdl", None), P("mdl", REP), P("mdl", REP))
    return jax.shard_map(body, mesh=torus, in_specs=in_specs, out_specs=out_specs, check_vma=False)
```

```python
import jax
import jax.numpy as jnp
from jax import lax
from jax.experimental import pallas as pl
from jax.experimental.pallas import tpu as pltpu
from jax.sharding import Mesh
from jax.sharding import PartitionSpec as P

REP = ("far", "near", "core")
PAIR = ("near", "core")
NODES = ("near", "mdl")
SWAP = [(0, 1), (1, 0)]
CHUNKS = 4
BLOCK = 16


highest = lax.Precision.HIGHEST
ANY = pl.BlockSpec(memory_space=pl.ANY)
HBM = pl.BlockSpec(memory_space=pltpu.HBM)
VMEM = pl.BlockSpec(memory_space=pltpu.VMEM)
SMEM = pl.BlockSpec(memory_space=pltpu.SMEM)
SMALL = pltpu.CompilerParams(vmem_limit_bytes=24 << 20)


def held(shape):
    return pltpu.VMEM(shape, jnp.float32)


def near_core(values):
    return pltpu.with_memory_space_constraint(values, pltpu.VMEM)


def far_off(values):
    return pltpu.with_memory_space_constraint(values, pltpu.HBM)


def pieces_of(values, count):
    found = []
    for _ in range(count):
        piece = values.astype(jnp.bfloat16)
        found.append(piece)
        values = values - piece.astype(jnp.float32)
    return found


def dot(a, b, dims):
    return lax.dot_general(a, b, (dims, ((), ())), preferred_element_type=jnp.float32)


def folded(stack, count):
    rows = stack.shape[0] // count
    return sum(stack[i * rows : (i + 1) * rows] for i in reversed(range(count)))


def pack(rows, out):
    share = out.shape[0]
    count = rows.shape[0] // share
    parts = [rows[i * share : (i + 1) * share] for i in range(count)]
    for i in range(count):
        out[:, i * 128 : (i + 1) * 128] = parts[i][:, :128]
    out[:, count * 128 :] = jnp.concatenate([part[:, 128:] for part in parts], axis=1)


def unpack(tiles, lanes):
    count = 128 // lanes
    heads = [tiles[:, i * 128 : (i + 1) * 128] for i in range(count)]
    tails = [tiles[:, count * 128 + i * lanes : count * 128 + (i + 1) * lanes] for i in range(count)]
    return jnp.concatenate([jnp.concatenate(heads, axis=0), jnp.concatenate(tails, axis=0)], axis=1)


def left_kernel(deltas, errors, starts, out, d_buf, e_buf, s_buf, sems):
    copies = [
        pltpu.make_async_copy(starts, s_buf, sems.at[0]),
        pltpu.make_async_copy(deltas, d_buf, sems.at[1]),
        pltpu.make_async_copy(errors, e_buf, sems.at[2]),
    ]
    for copy in copies:
        copy.start()
    copies[0].wait()
    stack = jnp.concatenate(pieces_of(s_buf[...], 3), axis=0)
    copies[1].wait()
    total = dot(stack, d_buf[0], ((1,), (1,)))
    copies[2].wait()
    total = folded(total + dot(stack, e_buf[0], ((1,), (1,))), 3)
    share = total.shape[0] // out.shape[0]
    for q in range(out.shape[0]):
        pack(total[q * share : (q + 1) * share], out.at[q])


def left_part_of(deltas, errors, starts):
    rows, columns = deltas.shape[1:]
    rank = starts.shape[0]
    pairs = lax.axis_size(PAIR)
    share = rank // pairs * (rows - 128) // 128
    return pl.pallas_call(
        left_kernel,
        out_shape=(
            held((pairs, share, rank // pairs * rows // share)),
            pltpu.VMEM(deltas.shape, jnp.bfloat16),
            pltpu.VMEM(errors.shape, jnp.bfloat16),
        ),
        in_specs=[HBM, HBM, HBM],
        out_specs=(VMEM, VMEM, VMEM),
        scratch_shapes=[held((rank, columns)), pltpu.SemaphoreType.DMA((3,))],
        compiler_params=SMALL,
        name="left_part",
    )(far_off(deltas), far_off(errors), far_off(starts))


def gram_lines(left, first, count):
    index = lax.broadcasted_iota(jnp.int32, left.shape, 0)
    own = [jnp.sum(jnp.where(index == first + i, left, 0.0), axis=0, keepdims=True) for i in range(count)]
    return lax.dot_general(
        jnp.concatenate(own, axis=0), left, (((1,), (1,)), ((), ())), precision=highest, preferred_element_type=jnp.float32
    )


def half_kernel(place, deltas, errors, out):
    width = out.shape[1]
    cut = pl.ds(pl.multiple_of((1 - place[0] % 2) * width, 128), width)
    out[...] = deltas[0, :, cut].astype(jnp.float32) + errors[0, :, cut].astype(jnp.float32)


def partner_half_of(place, deltas, errors):
    rows, columns = deltas.shape[1:]
    return pl.pallas_call(
        half_kernel,
        out_shape=held((rows, columns // 2)),
        in_specs=[SMEM, VMEM, VMEM],
        out_specs=VMEM,
        compiler_params=SMALL,
        cost_estimate=pl.CostEstimate(flops=40_000_000, transcendentals=0, bytes_accessed=2_000_000),
        name="partner_half",
    )(place, near_core(deltas), near_core(errors))


def right_kernel(place, quarters, partner, deltas, errors, out, left):
    rank, rows = left.shape
    share = out.shape[1]
    groups = rank // share
    width = out.shape[2] - rank
    whole = jnp.concatenate([unpack(quarters[q], rows - 128) for q in range(quarters.shape[0])], axis=0)
    left[...] = whole
    stack = jnp.concatenate(pieces_of(whole, 3), axis=0)
    base = place[0] % 2 * partner.shape[1]
    for j in range(out.shape[0] // groups):
        own = pl.ds(pl.multiple_of(base + j * width, 128), width)
        merged = deltas[0, :, own].astype(jnp.float32) + errors[0, :, own].astype(jnp.float32)
        part = None
        for piece in reversed(pieces_of(merged + partner[:, j * width : (j + 1) * width], 3)):
            term = dot(stack, piece, ((1,), (0,)))
            part = term if part is None else part + term
        part = folded(part, 3)
        for g in range(groups):
            out[j * groups + g, :, :width] = part[g * share : (g + 1) * share]
    lines = gram_lines(whole, place[0] // 2 * share, share)
    for p in range(out.shape[0]):
        out[p, :, width:] = lines


def right_part_of(place, quarters, partner, deltas, errors, rank):
    rows, width = partner.shape[0], partner.shape[1] // 2
    share = rank * 2 // lax.axis_size(NODES)
    return pl.pallas_call(
        right_kernel,
        out_shape=(held((rank * 2 // share, share, width + rank)), held((rank, rows))),
        in_specs=[SMEM, VMEM, VMEM, VMEM, VMEM],
        out_specs=(VMEM, VMEM),
        compiler_params=SMALL,
        name="right_part",
    )(place, near_core(quarters), near_core(partner), near_core(deltas), near_core(errors))


def lower_inverse_of(gram):
    rank = gram.shape[0]
    ident = jnp.where(
        lax.broadcasted_iota(jnp.int32, (rank, rank), 0) == lax.broadcasted_iota(jnp.int32, (rank, rank), 1), 1.0, 0.0
    )
    table = jnp.concatenate([gram, ident], axis=1)
    index = lax.broadcasted_iota(jnp.int32, table.shape, 0)
    for k in range(0, rank, BLOCK):
        cols = [jnp.broadcast_to(table[:, k + j : k + j + 1], table.shape) for j in range(BLOCK)]
        for j in range(BLOCK):
            at = k + j
            scale = 1.0 / cols[j][at : at + 1]
            ratio = jnp.where(index > at, cols[j] * scale, 0.0)
            for n in range(j + 1, BLOCK):
                cols[n] = cols[n] - ratio * cols[n][at : at + 1]
            line = table[at : at + 1]
            table = jnp.where(index == at, line * jnp.sqrt(scale), table - ratio * line)
    lane = lax.broadcasted_iota(jnp.int32, table.shape, 1)
    return jnp.where(lane < rank, pltpu.roll(table, rank, 1), table)


def factor_kernel(gram, left, out):
    rank = gram.shape[0]
    whole = left[...]
    inverse = lower_inverse_of(gram[...])
    basis = lax.dot_general(
        inverse[:, :rank], whole, (((1,), (0,)), ((), ())), precision=highest, preferred_element_type=jnp.float32
    )
    twice = lax.dot_general(
        basis, inverse, (((0,), (0,)), ((), ())), precision=highest, preferred_element_type=jnp.float32
    )
    out[...] = jnp.concatenate(pieces_of(twice, 2), axis=1)


def factor_of(gram, left):
    return pl.pallas_call(
        factor_kernel,
        out_shape=pltpu.VMEM((left.shape[1], 4 * gram.shape[0]), jnp.bfloat16),
        in_specs=[VMEM, VMEM],
        out_specs=VMEM,
        compiler_params=SMALL,
        cost_estimate=pl.CostEstimate(flops=40_000_000, transcendentals=0, bytes_accessed=200_000),
        name="factor",
    )(near_core(gram), near_core(left))


def product(flipped, right):
    big, small = pieces_of(right, 2)
    return dot(flipped, jnp.concatenate([big, small, big, small], axis=0), ((1,), (0,)))


def flatten(right, flat):
    share, width = right.shape[1:]
    groups = flat.shape[0] // share
    for j in range(right.shape[0] // groups):
        for g in range(groups):
            flat[g * share : (g + 1) * share, j * width : (j + 1) * width] = right[j * groups + g]


def residue(flipped, flat, deltas, errors, base, j, width):
    approx = product(flipped[...], flat[:, j * width : (j + 1) * width])
    cut = pl.ds(pl.multiple_of(base + j * width, 128), width)
    merged = deltas[0, :, cut].astype(jnp.float32) + errors[0, :, cut].astype(jnp.float32)
    return (merged - approx).astype(jnp.bfloat16)


def near_kernel(place, flipped, right, deltas, errors, out, flat):
    flatten(right, flat)
    half = flat.shape[1]
    width = half // (CHUNKS // 2)
    base = place[0] % 2 * half
    for j in range(CHUNKS // 2):
        out[:, j * width : (j + 1) * width] = residue(flipped, flat, deltas, errors, base, j, width)


def near_half_of(place, flipped, right, deltas, errors):
    rows, columns = deltas.shape[1:]
    rank = right.size * 2 // columns
    return pl.pallas_call(
        near_kernel,
        out_shape=(pltpu.VMEM((rows, columns // 2), jnp.bfloat16), held((rank, columns // 2))),
        in_specs=[SMEM, VMEM, VMEM, VMEM, VMEM],
        out_specs=(VMEM, VMEM),
        compiler_params=SMALL,
        cost_estimate=pl.CostEstimate(flops=40_000_000, transcendentals=0, bytes_accessed=2_000_000),
        name="near_half",
    )(place, near_core(flipped), near_core(right), near_core(deltas), near_core(errors))


def out_kernel(place, flipped, right, other, ready, deltas, errors, momentum, new_errors, new_momentum, outer_step, flat, buf, fresh, step, sems):
    half = right.shape[1]
    owned = momentum.shape[1]
    each = half // owned
    core = place[0] % 2
    own = pl.ds(pl.multiple_of(core * half, 128), half)
    copies = [pltpu.make_async_copy(ready, new_errors.at[0, :, own], sems.at[0])]
    copies[0].start()
    flatten(other, flat)
    width = half // (CHUNKS // 2)
    far = (1 - core) * half
    for j in range(CHUNKS // 2):
        cut = slice(j * width, (j + 1) * width)
        buf[:, cut] = residue(flipped, flat, deltas, errors, far, j, width)
        there = pl.ds(pl.multiple_of(far + j * width, 128), width)
        copy = pltpu.make_async_copy(buf.at[:, pl.ds(j * width, width)], new_errors.at[0, :, there], sems.at[3 + j])
        copy.start()
        copies.append(copy)
        if j == 0:
            first = place[0] % each * owned
            base = pl.multiple_of(jnp.minimum(first // 128, half // 128 - 2) * 128, 128)
            cut = pl.ds(base, 256)
            window = jnp.where(place[0] // each == core, right[:, cut], flat[:, cut])
            window = pltpu.roll(window, lax.rem(256 - (first - base), 256), 1)[:, :128]
            mine = product(flipped[...], window)[:, :owned]
            fresh[...] = 0.9 * momentum[...] + mine
            step[...] = 0.7 * (mine + 0.9 * fresh[...])
            for k, (source, target) in enumerate(((fresh, new_momentum), (step, outer_step))):
                copy = pltpu.make_async_copy(source, target, sems.at[1 + k])
                copy.start()
                copies.append(copy)
    for copy in copies:
        copy.wait()


def outputs_of(place, flipped, right, other, ready, deltas, errors, momentum):
    f32 = jnp.float32
    return pl.pallas_call(
        out_kernel,
        out_shape=(
            jax.ShapeDtypeStruct(deltas.shape, jnp.bfloat16),
            jax.ShapeDtypeStruct(momentum.shape, f32),
            jax.ShapeDtypeStruct(momentum.shape, f32),
        ),
        in_specs=[SMEM] + [VMEM] * 7,
        out_specs=(HBM, HBM, HBM),
        scratch_shapes=[
            held(right.shape),
            pltpu.VMEM(ready.shape, jnp.bfloat16),
            held(momentum.shape),
            held(momentum.shape),
            pltpu.SemaphoreType.DMA((3 + CHUNKS // 2,)),
        ],
        compiler_params=SMALL,
        name="outputs",
    )(place, *(near_core(a) for a in (flipped, right, other, ready, deltas, errors, momentum)))


def to_each(shard, axes):
    count = lax.axis_size(axes)
    return lax.all_to_all(
        jnp.broadcast_to(shard[None], (count, *shard.shape)), axes, 0, 0, tiled=True
    )


def body(deltas, errors, starts, momentum):
    replicas = lax.axis_size(REP)
    rank = starts.shape[1]
    place = lax.axis_index(REP)[None]
    load, deltas, errors = left_part_of(deltas, errors, starts.T)
    load, place = lax.optimization_barrier((load, place))
    own = lax.all_to_all(load, PAIR, 0, 0, tiled=True).sum(axis=0)
    own, spot = lax.optimization_barrier((own, place))
    other = partner_half_of(spot, deltas, errors)
    partner = lax.ppermute(other, "core", SWAP)
    own = to_each(own, "far")
    own = own.sum(axis=0) / replicas
    own, partner = lax.optimization_barrier((own, partner))
    quarters = to_each(own, PAIR).reshape(load.shape)
    load, left = right_part_of(place, quarters, partner, deltas, errors, rank)
    nodes = lax.axis_size(NODES)
    width = load.shape[2] - rank
    seen = lax.all_to_all(load, NODES, 0, 0, tiled=True)
    lines = seen[:, :, width:].reshape(lax.axis_size("near"), -1, *seen.shape[1:2], rank).sum(axis=1)
    far = to_each(jnp.concatenate([seen[:, :, :width].sum(axis=0), *lines], axis=1), "far")
    part = far[:, :, :width].sum(axis=0) / replicas
    right = to_each(part, NODES).reshape(nodes, -1, width)
    gram = jnp.moveaxis(far[:, :, width:].reshape(*far.shape[:2], -1, rank), 2, 1).reshape(rank, rank)
    flipped = factor_of(0.5 * (gram + gram.T), left)
    right, flipped = lax.optimization_barrier((right, flipped))
    other = lax.ppermute(right, "core", SWAP)
    ready, flat = near_half_of(place, flipped, right, deltas, errors)
    return outputs_of(place, flipped, flat, other, ready, deltas, errors, momentum)


def solution(mesh):
    torus = Mesh(mesh.devices.reshape(8, 2, 2, 16), ("far", "near", "core", "mdl"))
    in_specs = (P(REP, "mdl", None), P(REP, "mdl", None), P(), P("mdl", REP))
    out_specs = (P(REP, "mdl", None), P("mdl", REP), P("mdl", REP))
    return jax.shard_map(body, mesh=torus, in_specs=in_specs, out_specs=out_specs, check_vma=False)
```

```python
import jax
import jax.numpy as jnp
from jax import lax
from jax.experimental import pallas as pl
from jax.experimental.pallas import tpu as pltpu
from jax.sharding import Mesh
from jax.sharding import PartitionSpec as P

REP = ("far", "near", "core")
PAIR = ("near", "core")
NODES = ("near", "mdl")
SWAP = [(0, 1), (1, 0)]
CHUNKS = 4
BLOCK = 16


highest = lax.Precision.HIGHEST
ANY = pl.BlockSpec(memory_space=pl.ANY)
HBM = pl.BlockSpec(memory_space=pltpu.HBM)
VMEM = pl.BlockSpec(memory_space=pltpu.VMEM)
SMEM = pl.BlockSpec(memory_space=pltpu.SMEM)
SMALL = pltpu.CompilerParams(vmem_limit_bytes=24 << 20)


def held(shape):
    return pltpu.VMEM(shape, jnp.float32)


def near_core(values):
    return pltpu.with_memory_space_constraint(values, pltpu.VMEM)


def far_off(values):
    return pltpu.with_memory_space_constraint(values, pltpu.HBM)


def pieces_of(values, count):
    found = []
    for _ in range(count):
        piece = values.astype(jnp.bfloat16)
        found.append(piece)
        values = values - piece.astype(jnp.float32)
    return found


def dot(a, b, dims):
    return lax.dot_general(a, b, (dims, ((), ())), preferred_element_type=jnp.float32)


def folded(stack, count):
    rows = stack.shape[0] // count
    return sum(stack[i * rows : (i + 1) * rows] for i in reversed(range(count)))


def pack(rows, out):
    share = out.shape[0]
    count = rows.shape[0] // share
    parts = [rows[i * share : (i + 1) * share] for i in range(count)]
    for i in range(count):
        out[:, i * 128 : (i + 1) * 128] = parts[i][:, :128]
    out[:, count * 128 :] = jnp.concatenate([part[:, 128:] for part in parts], axis=1)


def unpack(tiles, lanes):
    count = 128 // lanes
    heads = [tiles[:, i * 128 : (i + 1) * 128] for i in range(count)]
    tails = [tiles[:, count * 128 + i * lanes : count * 128 + (i + 1) * lanes] for i in range(count)]
    return jnp.concatenate([jnp.concatenate(heads, axis=0), jnp.concatenate(tails, axis=0)], axis=1)


def left_kernel(deltas, errors, starts, out, d_buf, e_buf, s_buf, sems):
    copies = [
        pltpu.make_async_copy(starts, s_buf, sems.at[0]),
        pltpu.make_async_copy(deltas, d_buf, sems.at[1]),
        pltpu.make_async_copy(errors, e_buf, sems.at[2]),
    ]
    for copy in copies:
        copy.start()
    copies[0].wait()
    stack = jnp.concatenate(pieces_of(s_buf[...], 3), axis=0)
    copies[1].wait()
    total = dot(stack, d_buf[0], ((1,), (1,)))
    copies[2].wait()
    total = folded(total + dot(stack, e_buf[0], ((1,), (1,))), 3)
    share = total.shape[0] // out.shape[0]
    for q in range(out.shape[0]):
        pack(total[q * share : (q + 1) * share], out.at[q])


def left_part_of(deltas, errors, starts):
    rows, columns = deltas.shape[1:]
    rank = starts.shape[0]
    pairs = lax.axis_size(PAIR)
    share = rank // pairs * (rows - 128) // 128
    return pl.pallas_call(
        left_kernel,
        out_shape=(
            held((pairs, share, rank // pairs * rows // share)),
            pltpu.VMEM(deltas.shape, jnp.bfloat16),
            pltpu.VMEM(errors.shape, jnp.bfloat16),
        ),
        in_specs=[HBM, HBM, HBM],
        out_specs=(VMEM, VMEM, VMEM),
        scratch_shapes=[held((rank, columns)), pltpu.SemaphoreType.DMA((3,))],
        compiler_params=SMALL,
        name="left_part",
    )(far_off(deltas), far_off(errors), far_off(starts))


def gram_lines(left, first, count):
    index = lax.broadcasted_iota(jnp.int32, left.shape, 0)
    own = [jnp.sum(jnp.where(index == first + i, left, 0.0), axis=0, keepdims=True) for i in range(count)]
    return lax.dot_general(
        jnp.concatenate(own, axis=0), left, (((1,), (1,)), ((), ())), precision=highest, preferred_element_type=jnp.float32
    )


def half_kernel(place, deltas, errors, out):
    width = out.shape[1]
    cut = pl.ds(pl.multiple_of((1 - place[0] % 2) * width, 128), width)
    out[...] = deltas[0, :, cut].astype(jnp.float32) + errors[0, :, cut].astype(jnp.float32)


def partner_half_of(place, deltas, errors):
    rows, columns = deltas.shape[1:]
    return pl.pallas_call(
        half_kernel,
        out_shape=held((rows, columns // 2)),
        in_specs=[SMEM, VMEM, VMEM],
        out_specs=VMEM,
        compiler_params=SMALL,
        cost_estimate=pl.CostEstimate(flops=40_000_000, transcendentals=0, bytes_accessed=2_000_000),
        name="partner_half",
    )(place, near_core(deltas), near_core(errors))


def quarter_kernel(place, partner, deltas, errors, own, other):
    width = own.shape[1]
    near = place[0] // 2 % 2
    base = place[0] % 2 * partner.shape[1]
    for n, out in ((near, own), (1 - near, other)):
        cut = pl.ds(pl.multiple_of(base + n * width, 128), width)
        here = pl.ds(pl.multiple_of(n * width, 128), width)
        out[...] = (
            deltas[0, :, cut].astype(jnp.float32) + errors[0, :, cut].astype(jnp.float32) + partner[:, here]
        )


def quarters_of(place, partner, deltas, errors):
    rows, columns = partner.shape
    return pl.pallas_call(
        quarter_kernel,
        out_shape=(held((rows, columns // 2)), held((rows, columns // 2))),
        in_specs=[SMEM, VMEM, VMEM, VMEM],
        out_specs=(VMEM, VMEM),
        compiler_params=SMALL,
        name="merged_quarters",
    )(place, near_core(partner), near_core(deltas), near_core(errors))


def right_kernel(place, quarters, own, other, out, left):
    rank, rows = left.shape
    share = out.shape[1]
    groups = rank // share
    whole = jnp.concatenate([unpack(quarters[q], rows - 128) for q in range(quarters.shape[0])], axis=0)
    left[...] = whole
    stack = jnp.concatenate(pieces_of(whole, 3), axis=0)
    width = own.shape[1]
    part = None
    for piece in reversed(pieces_of(own[...] + other[...], 3)):
        term = dot(stack, piece, ((1,), (0,)))
        part = term if part is None else part + term
    part = folded(part, 3)
    for g in range(groups):
        out[g, :, :width] = part[g * share : (g + 1) * share]
    lines = gram_lines(whole, place[0] // 4 * 2 * share, 2 * share)
    for p in range(out.shape[0]):
        out[p, :, width : width + rank] = lines[:share]
        out[p, :, width + rank :] = lines[share:]


def right_part_of(place, quarters, own, other, rank):
    rows, width = own.shape
    groups = lax.axis_size("mdl")
    return pl.pallas_call(
        right_kernel,
        out_shape=(held((groups, rank // groups, width + 2 * rank)), held((rank, rows))),
        in_specs=[SMEM, VMEM, VMEM, VMEM],
        out_specs=(VMEM, VMEM),
        compiler_params=SMALL,
        name="right_part",
    )(place, near_core(quarters), near_core(own), near_core(other))


def lower_inverse_of(gram):
    rank = gram.shape[0]
    ident = jnp.where(
        lax.broadcasted_iota(jnp.int32, (rank, rank), 0) == lax.broadcasted_iota(jnp.int32, (rank, rank), 1), 1.0, 0.0
    )
    table = jnp.concatenate([gram, ident], axis=1)
    index = lax.broadcasted_iota(jnp.int32, table.shape, 0)
    for k in range(0, rank, BLOCK):
        cols = [jnp.broadcast_to(table[:, k + j : k + j + 1], table.shape) for j in range(BLOCK)]
        for j in range(BLOCK):
            at = k + j
            scale = 1.0 / cols[j][at : at + 1]
            ratio = jnp.where(index > at, cols[j] * scale, 0.0)
            for n in range(j + 1, BLOCK):
                cols[n] = cols[n] - ratio * cols[n][at : at + 1]
            line = table[at : at + 1]
            table = jnp.where(index == at, line * jnp.sqrt(scale), table - ratio * line)
    lane = lax.broadcasted_iota(jnp.int32, table.shape, 1)
    return jnp.where(lane < rank, pltpu.roll(table, rank, 1), table)


def factor_kernel(gram, left, out):
    rank = gram.shape[0]
    whole = left[...]
    inverse = lower_inverse_of(gram[...])
    basis = lax.dot_general(
        inverse[:, :rank], whole, (((1,), (0,)), ((), ())), precision=highest, preferred_element_type=jnp.float32
    )
    twice = lax.dot_general(
        basis, inverse, (((0,), (0,)), ((), ())), precision=highest, preferred_element_type=jnp.float32
    )
    out[...] = jnp.concatenate(pieces_of(twice, 2), axis=1)


def factor_of(gram, left):
    return pl.pallas_call(
        factor_kernel,
        out_shape=pltpu.VMEM((left.shape[1], 4 * gram.shape[0]), jnp.bfloat16),
        in_specs=[VMEM, VMEM],
        out_specs=VMEM,
        compiler_params=SMALL,
        cost_estimate=pl.CostEstimate(flops=40_000_000, transcendentals=0, bytes_accessed=200_000),
        name="factor",
    )(near_core(gram), near_core(left))


def product(flipped, right):
    big, small = pieces_of(right, 2)
    return dot(flipped, jnp.concatenate([big, small, big, small], axis=0), ((1,), (0,)))


def flatten(right, flat):
    share, width = right.shape[1:]
    groups = flat.shape[0] // share
    for j in range(right.shape[0] // groups):
        for g in range(groups):
            flat[g * share : (g + 1) * share, j * width : (j + 1) * width] = right[j * groups + g]


def residue(flipped, flat, deltas, errors, base, j, width):
    approx = product(flipped[...], flat[:, j * width : (j + 1) * width])
    cut = pl.ds(pl.multiple_of(base + j * width, 128), width)
    merged = deltas[0, :, cut].astype(jnp.float32) + errors[0, :, cut].astype(jnp.float32)
    return (merged - approx).astype(jnp.bfloat16)


def near_kernel(place, flipped, right, deltas, errors, out, flat):
    flatten(right, flat)
    half = flat.shape[1]
    width = half // (CHUNKS // 2)
    base = place[0] % 2 * half
    for j in range(CHUNKS // 2):
        out[:, j * width : (j + 1) * width] = residue(flipped, flat, deltas, errors, base, j, width)


def near_half_of(place, flipped, right, deltas, errors):
    rows, columns = deltas.shape[1:]
    rank = right.size * 2 // columns
    return pl.pallas_call(
        near_kernel,
        out_shape=(pltpu.VMEM((rows, columns // 2), jnp.bfloat16), held((rank, columns // 2))),
        in_specs=[SMEM, VMEM, VMEM, VMEM, VMEM],
        out_specs=(VMEM, VMEM),
        compiler_params=SMALL,
        cost_estimate=pl.CostEstimate(flops=40_000_000, transcendentals=0, bytes_accessed=2_000_000),
        name="near_half",
    )(place, near_core(flipped), near_core(right), near_core(deltas), near_core(errors))


def out_kernel(place, flipped, right, other, ready, deltas, errors, momentum, new_errors, new_momentum, outer_step, flat, buf, fresh, step, sems):
    half = right.shape[1]
    owned = momentum.shape[1]
    each = half // owned
    core = place[0] % 2
    own = pl.ds(pl.multiple_of(core * half, 128), half)
    copies = [pltpu.make_async_copy(ready, new_errors.at[0, :, own], sems.at[0])]
    copies[0].start()
    flatten(other, flat)
    width = half // (CHUNKS // 2)
    far = (1 - core) * half
    for j in range(CHUNKS // 2):
        cut = slice(j * width, (j + 1) * width)
        buf[:, cut] = residue(flipped, flat, deltas, errors, far, j, width)
        there = pl.ds(pl.multiple_of(far + j * width, 128), width)
        copy = pltpu.make_async_copy(buf.at[:, pl.ds(j * width, width)], new_errors.at[0, :, there], sems.at[3 + j])
        copy.start()
        copies.append(copy)
        if j == 0:
            first = place[0] % each * owned
            base = pl.multiple_of(jnp.minimum(first // 128, half // 128 - 2) * 128, 128)
            cut = pl.ds(base, 256)
            window = jnp.where(place[0] // each == core, right[:, cut], flat[:, cut])
            window = pltpu.roll(window, lax.rem(256 - (first - base), 256), 1)[:, :128]
            mine = product(flipped[...], window)[:, :owned]
            fresh[...] = 0.9 * momentum[...] + mine
            step[...] = 0.7 * (mine + 0.9 * fresh[...])
            for k, (source, target) in enumerate(((fresh, new_momentum), (step, outer_step))):
                copy = pltpu.make_async_copy(source, target, sems.at[1 + k])
                copy.start()
                copies.append(copy)
    for copy in copies:
        copy.wait()


def outputs_of(place, flipped, right, other, ready, deltas, errors, momentum):
    f32 = jnp.float32
    return pl.pallas_call(
        out_kernel,
        out_shape=(
            jax.ShapeDtypeStruct(deltas.shape, jnp.bfloat16),
            jax.ShapeDtypeStruct(momentum.shape, f32),
            jax.ShapeDtypeStruct(momentum.shape, f32),
        ),
        in_specs=[SMEM] + [VMEM] * 7,
        out_specs=(HBM, HBM, HBM),
        scratch_shapes=[
            held(right.shape),
            pltpu.VMEM(ready.shape, jnp.bfloat16),
            held(momentum.shape),
            held(momentum.shape),
            pltpu.SemaphoreType.DMA((3 + CHUNKS // 2,)),
        ],
        compiler_params=SMALL,
        name="outputs",
    )(place, *(near_core(a) for a in (flipped, right, other, ready, deltas, errors, momentum)))


def to_each(shard, axes):
    count = lax.axis_size(axes)
    return lax.all_to_all(
        jnp.broadcast_to(shard[None], (count, *shard.shape)), axes, 0, 0, tiled=True
    )


def body(deltas, errors, starts, momentum):
    replicas = lax.axis_size(REP)
    rank = starts.shape[1]
    place = lax.axis_index(REP)[None]
    load, deltas, errors = left_part_of(deltas, errors, starts.T)
    load, place = lax.optimization_barrier((load, place))
    own = lax.all_to_all(load, PAIR, 0, 0, tiled=True).sum(axis=0)
    own, spot = lax.optimization_barrier((own, place))
    other = partner_half_of(spot, deltas, errors)
    partner = lax.ppermute(other, "core", SWAP)
    own = to_each(own, "far")
    own = own.sum(axis=0) / replicas
    mine, other = quarters_of(place, partner, deltas, errors)
    other = lax.ppermute(other, "near", SWAP)
    quarters = to_each(own, PAIR).reshape(load.shape)
    load, left = right_part_of(place, quarters, mine, other, rank)
    nodes = lax.axis_size(NODES)
    width = load.shape[2] - 2 * rank
    total = lax.all_to_all(load, "mdl", 0, 0, tiled=True).sum(axis=0)
    far = to_each(total, "far")
    part = far[:, :, :width].sum(axis=0) / replicas
    right = to_each(part, NODES).reshape(nodes, -1, width)
    gram = jnp.moveaxis(far[:, :, width:].reshape(*far.shape[:2], -1, rank), 2, 1).reshape(rank, rank)
    flipped = factor_of(0.5 * (gram + gram.T), left)
    right, flipped = lax.optimization_barrier((right, flipped))
    other = lax.ppermute(right, "core", SWAP)
    ready, flat = near_half_of(place, flipped, right, deltas, errors)
    return outputs_of(place, flipped, flat, other, ready, deltas, errors, momentum)


def solution(mesh):
    torus = Mesh(mesh.devices.reshape(8, 2, 2, 16), ("far", "near", "core", "mdl"))
    in_specs = (P(REP, "mdl", None), P(REP, "mdl", None), P(), P("mdl", REP))
    out_specs = (P(REP, "mdl", None), P("mdl", REP), P("mdl", REP))
    return jax.shard_map(body, mesh=torus, in_specs=in_specs, out_specs=out_specs, check_vma=False)
```

```python
import jax
import jax.numpy as jnp
from jax import lax
from jax.experimental import pallas as pl
from jax.experimental.pallas import tpu as pltpu
from jax.sharding import Mesh
from jax.sharding import PartitionSpec as P

REP = ("far", "near", "core")
PAIR = ("near", "core")
NODES = ("near", "mdl")
SWAP = [(0, 1), (1, 0)]
CHUNKS = 10
BLOCK = 16


highest = lax.Precision.HIGHEST
ANY = pl.BlockSpec(memory_space=pl.ANY)
HBM = pl.BlockSpec(memory_space=pltpu.HBM)
VMEM = pl.BlockSpec(memory_space=pltpu.VMEM)
SMEM = pl.BlockSpec(memory_space=pltpu.SMEM)
SMALL = pltpu.CompilerParams(vmem_limit_bytes=24 << 20)


def held(shape):
    return pltpu.VMEM(shape, jnp.float32)


def near_core(values):
    return pltpu.with_memory_space_constraint(values, pltpu.VMEM)


def far_off(values):
    return pltpu.with_memory_space_constraint(values, pltpu.HBM)


def pieces_of(values, count):
    found = []
    for _ in range(count):
        piece = values.astype(jnp.bfloat16)
        found.append(piece)
        values = values - piece.astype(jnp.float32)
    return found


def dot(a, b, dims):
    return lax.dot_general(a, b, (dims, ((), ())), preferred_element_type=jnp.float32)


def folded(stack, count):
    rows = stack.shape[0] // count
    return sum(stack[i * rows : (i + 1) * rows] for i in reversed(range(count)))


def pack(rows, out):
    share = out.shape[0]
    count = rows.shape[0] // share
    parts = [rows[i * share : (i + 1) * share] for i in range(count)]
    for i in range(count):
        out[:, i * 128 : (i + 1) * 128] = parts[i][:, :128]
    out[:, count * 128 :] = jnp.concatenate([part[:, 128:] for part in parts], axis=1)


def unpack(tiles, lanes):
    count = 128 // lanes
    heads = [tiles[:, i * 128 : (i + 1) * 128] for i in range(count)]
    tails = [tiles[:, count * 128 + i * lanes : count * 128 + (i + 1) * lanes] for i in range(count)]
    return jnp.concatenate([jnp.concatenate(heads, axis=0), jnp.concatenate(tails, axis=0)], axis=1)


def left_kernel(deltas, errors, starts, out, d_buf, e_buf, s_buf, sems):
    copies = [
        pltpu.make_async_copy(starts, s_buf, sems.at[0]),
        pltpu.make_async_copy(deltas, d_buf, sems.at[1]),
        pltpu.make_async_copy(errors, e_buf, sems.at[2]),
    ]
    for copy in copies:
        copy.start()
    copies[0].wait()
    stack = jnp.concatenate(pieces_of(s_buf[...], 3), axis=0)
    copies[1].wait()
    total = dot(stack, d_buf[0], ((1,), (1,)))
    copies[2].wait()
    total = folded(total + dot(stack, e_buf[0], ((1,), (1,))), 3)
    share = total.shape[0] // out.shape[0]
    for q in range(out.shape[0]):
        pack(total[q * share : (q + 1) * share], out.at[q])


def left_part_of(deltas, errors, starts):
    rows, columns = deltas.shape[1:]
    rank = starts.shape[0]
    pairs = lax.axis_size(PAIR)
    share = rank // pairs * (rows - 128) // 128
    return pl.pallas_call(
        left_kernel,
        out_shape=(
            held((pairs, share, rank // pairs * rows // share)),
            pltpu.VMEM(deltas.shape, jnp.bfloat16),
            pltpu.VMEM(errors.shape, jnp.bfloat16),
        ),
        in_specs=[HBM, HBM, HBM],
        out_specs=(VMEM, VMEM, VMEM),
        scratch_shapes=[held((rank, columns)), pltpu.SemaphoreType.DMA((3,))],
        compiler_params=SMALL,
        name="left_part",
    )(far_off(deltas), far_off(errors), far_off(starts))


def gram_lines(left, first, count):
    index = lax.broadcasted_iota(jnp.int32, left.shape, 0)
    own = [jnp.sum(jnp.where(index == first + i, left, 0.0), axis=0, keepdims=True) for i in range(count)]
    return lax.dot_general(
        jnp.concatenate(own, axis=0), left, (((1,), (1,)), ((), ())), precision=highest, preferred_element_type=jnp.float32
    )


def half_kernel(place, deltas, errors, out):
    width = out.shape[1]
    cut = pl.ds(pl.multiple_of((1 - place[0] % 2) * width, 128), width)
    out[...] = deltas[0, :, cut].astype(jnp.float32) + errors[0, :, cut].astype(jnp.float32)


def partner_half_of(place, deltas, errors):
    rows, columns = deltas.shape[1:]
    return pl.pallas_call(
        half_kernel,
        out_shape=held((rows, columns // 2)),
        in_specs=[SMEM, VMEM, VMEM],
        out_specs=VMEM,
        compiler_params=SMALL,
        cost_estimate=pl.CostEstimate(flops=40_000_000, transcendentals=0, bytes_accessed=2_000_000),
        name="partner_half",
    )(place, near_core(deltas), near_core(errors))


def right_kernel(place, quarters, partner, deltas, errors, out, left):
    rank, rows = left.shape
    share = out.shape[1]
    groups = rank // share
    width = out.shape[2] - rank
    whole = jnp.concatenate([unpack(quarters[q], rows - 128) for q in range(quarters.shape[0])], axis=0)
    left[...] = whole
    stack = jnp.concatenate(pieces_of(whole, 3), axis=0)
    base = place[0] % 2 * partner.shape[1]
    for j in range(out.shape[0] // groups):
        own = pl.ds(pl.multiple_of(base + j * width, 128), width)
        merged = deltas[0, :, own].astype(jnp.float32) + errors[0, :, own].astype(jnp.float32)
        part = None
        for piece in reversed(pieces_of(merged + partner[:, j * width : (j + 1) * width], 3)):
            term = dot(stack, piece, ((1,), (0,)))
            part = term if part is None else part + term
        part = folded(part, 3)
        for g in range(groups):
            out[j * groups + g, :, :width] = part[g * share : (g + 1) * share]
    lines = gram_lines(whole, place[0] // 2 * share, share)
    for p in range(out.shape[0]):
        out[p, :, width:] = lines


def right_part_of(place, quarters, partner, deltas, errors, rank):
    rows, width = partner.shape[0], partner.shape[1] // 2
    share = rank * 2 // lax.axis_size(NODES)
    return pl.pallas_call(
        right_kernel,
        out_shape=(held((rank * 2 // share, share, width + rank)), held((rank, rows))),
        in_specs=[SMEM, VMEM, VMEM, VMEM, VMEM],
        out_specs=(VMEM, VMEM),
        compiler_params=SMALL,
        name="right_part",
    )(place, near_core(quarters), near_core(partner), near_core(deltas), near_core(errors))


def lower_inverse_of(gram):
    rank = gram.shape[0]
    ident = jnp.where(
        lax.broadcasted_iota(jnp.int32, (rank, rank), 0) == lax.broadcasted_iota(jnp.int32, (rank, rank), 1), 1.0, 0.0
    )
    table = jnp.concatenate([gram, ident], axis=1)
    index = lax.broadcasted_iota(jnp.int32, table.shape, 0)
    for k in range(0, rank, BLOCK):
        cols = [jnp.broadcast_to(table[:, k + j : k + j + 1], table.shape) for j in range(BLOCK)]
        for j in range(BLOCK):
            at = k + j
            scale = 1.0 / cols[j][at : at + 1]
            ratio = jnp.where(index > at, cols[j] * scale, 0.0)
            for n in range(j + 1, BLOCK):
                cols[n] = cols[n] - ratio * cols[n][at : at + 1]
            line = table[at : at + 1]
            table = jnp.where(index == at, line * jnp.sqrt(scale), table - ratio * line)
    lane = lax.broadcasted_iota(jnp.int32, table.shape, 1)
    return jnp.where(lane < rank, pltpu.roll(table, rank, 1), table)


def factor_kernel(gram, left, out):
    rank = gram.shape[0]
    whole = left[...]
    inverse = lower_inverse_of(gram[...])
    basis = lax.dot_general(
        inverse[:, :rank], whole, (((1,), (0,)), ((), ())), precision=highest, preferred_element_type=jnp.float32
    )
    twice = lax.dot_general(
        basis, inverse, (((0,), (0,)), ((), ())), precision=highest, preferred_element_type=jnp.float32
    )
    out[...] = jnp.concatenate(pieces_of(twice, 2), axis=1)


def factor_of(gram, left):
    return pl.pallas_call(
        factor_kernel,
        out_shape=pltpu.VMEM((left.shape[1], 4 * gram.shape[0]), jnp.bfloat16),
        in_specs=[VMEM, VMEM],
        out_specs=VMEM,
        compiler_params=SMALL,
        cost_estimate=pl.CostEstimate(flops=40_000_000, transcendentals=0, bytes_accessed=200_000),
        name="factor",
    )(near_core(gram), near_core(left))


def product(flipped, right):
    big, small = pieces_of(right, 2)
    return dot(flipped, jnp.concatenate([big, small, big, small], axis=0), ((1,), (0,)))


def flatten(right, flat):
    share, width = right.shape[1:]
    groups = flat.shape[0] // share
    for j in range(right.shape[0] // groups):
        for g in range(groups):
            flat[g * share : (g + 1) * share, j * width : (j + 1) * width] = right[j * groups + g]


def residue(flipped, flat, deltas, errors, base, j, width):
    approx = product(flipped[...], flat[:, j * width : (j + 1) * width])
    cut = pl.ds(pl.multiple_of(base + j * width, 128), width)
    merged = deltas[0, :, cut].astype(jnp.float32) + errors[0, :, cut].astype(jnp.float32)
    return (merged - approx).astype(jnp.bfloat16)


def near_kernel(place, flipped, right, deltas, errors, new_errors, flat, buf, sems):
    flatten(right, flat)
    half = flat.shape[1]
    width = half // (CHUNKS // 2)
    base = place[0] % 2 * half
    copies = []
    for j in range(CHUNKS // 2):
        buf[:, j * width : (j + 1) * width] = residue(flipped, flat, deltas, errors, base, j, width)
        there = pl.ds(pl.multiple_of(base + j * width, 128), width)
        copy = pltpu.make_async_copy(buf.at[:, pl.ds(j * width, width)], new_errors.at[0, :, there], sems.at[j])
        copy.start()
        copies.append(copy)
    for copy in copies:
        copy.wait()


def near_half_of(place, flipped, right, deltas, errors):
    rows, columns = deltas.shape[1:]
    rank = right.size * 2 // columns
    return pl.pallas_call(
        near_kernel,
        out_shape=(jax.ShapeDtypeStruct(deltas.shape, jnp.bfloat16), held((rank, columns // 2))),
        in_specs=[SMEM, VMEM, VMEM, VMEM, VMEM],
        out_specs=(HBM, VMEM),
        scratch_shapes=[pltpu.VMEM((rows, columns // 2), jnp.bfloat16), pltpu.SemaphoreType.DMA((CHUNKS // 2,))],
        compiler_params=SMALL,
        cost_estimate=pl.CostEstimate(flops=40_000_000, transcendentals=0, bytes_accessed=2_000_000),
        name="near_half",
    )(place, near_core(flipped), near_core(right), near_core(deltas), near_core(errors))


def out_kernel(place, flipped, right, other, ready, deltas, errors, momentum, new_errors, new_momentum, outer_step, flat, buf, fresh, step, sems):
    half = right.shape[1]
    owned = momentum.shape[1]
    each = half // owned
    core = place[0] % 2
    copies = []
    flatten(other, flat)
    width = half // (CHUNKS // 2)
    far = (1 - core) * half
    for j in range(CHUNKS // 2):
        cut = slice(j * width, (j + 1) * width)
        buf[:, cut] = residue(flipped, flat, deltas, errors, far, j, width)
        there = pl.ds(pl.multiple_of(far + j * width, 128), width)
        copy = pltpu.make_async_copy(buf.at[:, pl.ds(j * width, width)], new_errors.at[0, :, there], sems.at[2 + j])
        copy.start()
        copies.append(copy)
        if j == 0:
            first = place[0] % each * owned
            base = pl.multiple_of(jnp.minimum(first // 128, half // 128 - 2) * 128, 128)
            cut = pl.ds(base, 256)
            window = jnp.where(place[0] // each == core, right[:, cut], flat[:, cut])
            window = pltpu.roll(window, lax.rem(256 - (first - base), 256), 1)[:, :128]
            mine = product(flipped[...], window)[:, :owned]
            fresh[...] = 0.9 * momentum[...] + mine
            step[...] = 0.7 * (mine + 0.9 * fresh[...])
            for k, (source, target) in enumerate(((fresh, new_momentum), (step, outer_step))):
                copy = pltpu.make_async_copy(source, target, sems.at[k])
                copy.start()
                copies.append(copy)
    for copy in copies:
        copy.wait()


def outputs_of(place, flipped, right, other, ready, deltas, errors, momentum):
    f32 = jnp.float32
    return pl.pallas_call(
        out_kernel,
        out_shape=(
            jax.ShapeDtypeStruct(deltas.shape, jnp.bfloat16),
            jax.ShapeDtypeStruct(momentum.shape, f32),
            jax.ShapeDtypeStruct(momentum.shape, f32),
        ),
        in_specs=[SMEM] + [VMEM] * 3 + [HBM] + [VMEM] * 3,
        input_output_aliases={4: 0},
        out_specs=(HBM, HBM, HBM),
        scratch_shapes=[
            held(right.shape),
            pltpu.VMEM((momentum.shape[0], right.shape[1]), jnp.bfloat16),
            held(momentum.shape),
            held(momentum.shape),
            pltpu.SemaphoreType.DMA((2 + CHUNKS // 2,)),
        ],
        compiler_params=SMALL,
        name="outputs",
    )(place, *map(near_core, (flipped, right, other)), far_off(ready), *map(near_core, (deltas, errors, momentum)))


def to_each(shard, axes):
    count = lax.axis_size(axes)
    return lax.all_to_all(
        jnp.broadcast_to(shard[None], (count, *shard.shape)), axes, 0, 0, tiled=True
    )


def body(deltas, errors, starts, momentum):
    replicas = lax.axis_size(REP)
    rank = starts.shape[1]
    place = lax.axis_index(REP)[None]
    load, deltas, errors = left_part_of(deltas, errors, starts.T)
    load, place = lax.optimization_barrier((load, place))
    own = lax.all_to_all(load, PAIR, 0, 0, tiled=True).sum(axis=0)
    own, spot = lax.optimization_barrier((own, place))
    other = partner_half_of(spot, deltas, errors)
    partner = lax.ppermute(other, "core", SWAP)
    own = to_each(own, "far")
    own = own.sum(axis=0) / replicas
    own, partner = lax.optimization_barrier((own, partner))
    quarters = to_each(own, PAIR).reshape(load.shape)
    load, left = right_part_of(place, quarters, partner, deltas, errors, rank)
    nodes = lax.axis_size(NODES)
    width = load.shape[2] - rank
    seen = lax.all_to_all(load, NODES, 0, 0, tiled=True)
    lines = seen[:, :, width:].reshape(lax.axis_size("near"), -1, *seen.shape[1:2], rank).sum(axis=1)
    far = to_each(jnp.concatenate([seen[:, :, :width].sum(axis=0), *lines], axis=1), "far")
    part = far[:, :, :width].sum(axis=0) / replicas
    right = to_each(part, NODES).reshape(nodes, -1, width)
    gram = jnp.moveaxis(far[:, :, width:].reshape(*far.shape[:2], -1, rank), 2, 1).reshape(rank, rank)
    flipped = factor_of(0.5 * (gram + gram.T), left)
    right, flipped = lax.optimization_barrier((right, flipped))
    other = lax.ppermute(right, "core", SWAP)
    ready, flat = near_half_of(place, flipped, right, deltas, errors)
    return outputs_of(place, flipped, flat, other, ready, deltas, errors, momentum)


def solution(mesh):
    torus = Mesh(mesh.devices.reshape(8, 2, 2, 16), ("far", "near", "core", "mdl"))
    in_specs = (P(REP, "mdl", None), P(REP, "mdl", None), P(), P("mdl", REP))
    out_specs = (P(REP, "mdl", None), P("mdl", REP), P("mdl", REP))
    return jax.shard_map(body, mesh=torus, in_specs=in_specs, out_specs=out_specs, check_vma=False)
```
